8 devices in a mesh: dp: 2 (over y, z), tp: 4 (over x, core).
Axes of the slice: x: 2, y: 2, z: 1, core: 2. Of those that a mesh axis runs over, the one named last changes fastest.
Arguments:
- x: bfloat16 [128, 4096], P('dp'), parts along dimension 0
- k_cache: bfloat16 [128, 2048, 8, 128], P('dp', None, 'tp'), parts along dimension 0
- v_cache: bfloat16 [128, 2048, 8, 128], P('dp', None, 'tp'), parts along dimension 0
- gain_a: bfloat16 [4096], replicated
- wq: bfloat16 [4096, 4096], P(None, 'tp')
- wo: bfloat16 [4096, 4096], P('tp')
- gain_m: bfloat16 [4096], replicated
- w_gate: bfloat16 [4096, 14336], P(None, 'tp')
- w_up: bfloat16 [4096, 14336], P(None, 'tp')
- w_down: bfloat16 [14336, 4096], P('tp')
Outputs:
- output: bfloat16 [128, 4096], P('dp'), parts along dimension 0
There are 2 independent parts. The reference program is written for one: setup_inputs(seed, part) draws one part's arguments, and reference() takes and returns one part's arrays. A program takes and returns all parts, laid end to end along the dimension named above; an argument that names none is the same for every part.
All inputs are finite; a program needn't handle non-finite values.
Results may differ from the reference program's by a relative error of at most 0.017.
Values are sent between devices in bfloat16 or wider.
A program may use at most 2 GiB of HBM per device.

```python
import jax
import jax.numpy as jnp
from jax import lax

BATCH = 64
CACHE = 2048
D = 4096
HEADS = 32
KV_HEADS = 8
HEAD = 128
FF = 14336
THETA = 10000


def setup_inputs(seed: int = 0, part: int = 0) -> dict:
    kx, kc, kw, kn, kq, ko, km, kg, ku, kd = jax.random.split(jax.random.key(seed), 10)
    kx, kc, kw = (jax.random.fold_in(k, part) for k in (kx, kc, kw))

    def weights(key, rows, columns):
        return jax.random.normal(key, (rows, columns), jnp.float32) * rows**-0.5

    drawn = {
        "x": jax.random.normal(kx, (BATCH, D), jnp.float32),
        "k_cache": 2 * jax.random.normal(kc, (BATCH, CACHE, KV_HEADS, HEAD), jnp.float32),
        "v_cache": 4 * jax.random.normal(kw, (BATCH, CACHE, KV_HEADS, HEAD), jnp.float32),
        "gain_a": 1 + 0.1 * jax.random.normal(kn, (D,), jnp.float32),
        "wq": 2 * weights(kq, D, HEADS * HEAD),
        "wo": weights(ko, HEADS * HEAD, D),
        "gain_m": 1 + 0.1 * jax.random.normal(km, (D,), jnp.float32),
        "w_gate": weights(kg, D, FF),
        "w_up": weights(ku, D, FF),
        "w_down": 2 * weights(kd, FF, D),
    }
    return {k: v.astype(jnp.bfloat16) for k, v in drawn.items()}


def normed(x, gain):
    wide = x.astype(jnp.float32)
    scale = lax.rsqrt(jnp.mean(wide * wide, -1, keepdims=True) + 1e-6)
    return (wide * scale * gain.astype(jnp.float32)).astype(jnp.bfloat16)


def turned(t, place, theta):
    half = t.shape[-1] // 2
    angle = place.astype(jnp.float32)[:, None] * theta ** (-jnp.arange(half, dtype=jnp.float32) / half)
    cos, sin = jnp.cos(angle)[:, None], jnp.sin(angle)[:, None]
    a, b = t[..., :half].astype(jnp.float32), t[..., half:].astype(jnp.float32)
    return jnp.concatenate([a * cos - b * sin, b * cos + a * sin], -1).astype(jnp.bfloat16)


def matmul(a, w):
    return jnp.dot(a, w, preferred_element_type=jnp.float32).astype(jnp.bfloat16)


def einsum(form, a, b):
    return jnp.einsum(form, a.astype(jnp.float32), b.astype(jnp.float32))


def seen_by(a, wq, k_cache, v_cache, head, theta):
    batch, cache, kv_heads = k_cache.shape[:3]
    place = jnp.full((batch,), cache - 1)
    q = turned(matmul(a, wq).reshape(batch, -1, head), place, theta).reshape(batch, kv_heads, -1, head)
    scores = einsum("bgsd,bugd->bgsu", q, k_cache) * head**-0.5
    weights = jax.nn.softmax(scores, -1).astype(jnp.bfloat16)
    return einsum("bgsu,bugd->bgsd", weights, v_cache).astype(jnp.bfloat16).reshape(batch, -1)


def hidden_of(b, w_gate, w_up):
    gate = jnp.dot(b, w_gate, preferred_element_type=jnp.float32)
    up = jnp.dot(b, w_up, preferred_element_type=jnp.float32)
    return (jax.nn.silu(gate) * up).astype(jnp.bfloat16)


def reference(x, k_cache, v_cache, gain_a, wq, wo, gain_m, w_gate, w_up, w_down):
    seen = seen_by(normed(x, gain_a), wq, k_cache, v_cache, HEAD, THETA)
    h = (x.astype(jnp.float32) + jnp.dot(seen, wo, preferred_element_type=jnp.float32)).astype(jnp.bfloat16)
    hidden = hidden_of(normed(h, gain_m), w_gate, w_up)
    return (h.astype(jnp.float32) + jnp.dot(hidden, w_down, preferred_element_type=jnp.float32)).astype(jnp.bfloat16)
```

```python
import jax
import jax.numpy as jnp
import numpy as np
from jax import lax
from jax.experimental import pallas as pl
from jax.experimental.pallas import tpu as pltpu
from jax.sharding import PartitionSpec as P

HEAD = 128
THETA = 10000
BATCH = 64
CACHE = 2048
KV = 2
D = 4096
FF = 3584
ROWS, COLS = 1024, 512
SB = 4
R = 12
GROUPS = BATCH // SB
TILE = 256
NT = D // TILE
NB = D // COLS
NF = FF // COLS
Q_K0, Q_KV, Q_VL, Q_WO, Q_GU, Q_WD = 2, 3, 33, 34, 36, 50
F32, BF16 = jnp.float32, jnp.bfloat16
NEG = float("-inf")


def kernel(x_hbm, k_hbm, v_hbm, ga_hbm, wq, wo, gm_hbm, wg, wu, wd, rot_hbm, out,
           ring, xb, ab, gb, rb, qb, sca, scb, seen, hid, f1, s1, r1, s2, r2, y,
           sem, xsem, gsem, ss1, rs1, ss2, rs2, ss3, rs3, osem):
    tp = lax.axis_index("tp")
    k = lax.rem(tp, 2)
    sib = tp + 1 - 2 * k
    far = lax.rem(tp + 2, 4)

    def slot(quad, s):
        return (quad % R if isinstance(quad, int) else lax.rem(quad, R)) * SB + s

    def put(src, dst, s):
        pltpu.make_async_copy(src, dst, s).start()

    def issue_wq(nc):
        for s in range(SB):
            i = slot(nc, s)
            put(wq.at[pl.ds(s * ROWS, ROWS), pl.ds(nc * COLS, COLS)], ring.at[i], sem.at[i])

    def issue_kv(ref, g, quad):
        for s in range(SB):
            i = slot(quad, s)
            for c in range(4):
                put(ref.at[g * SB + s, pl.ds(c * ROWS, ROWS), :], ring.at[i, :, pl.ds(c * 128, 128)], sem.at[i])

    def issue_wo(q):
        for s in range(SB):
            i = slot(Q_WO + q, s)
            put(wo.at[:, pl.ds((q * SB + s) * COLS, COLS)], ring.at[i], sem.at[i])

    def issue_gu(ref, nb, quad):
        for s in range(SB):
            i = slot(quad, s)
            cols = pl.ds(nb * COLS if isinstance(nb, int) else pl.multiple_of(nb * COLS, COLS), COLS)
            put(ref.at[pl.ds(s * ROWS, ROWS), cols], ring.at[i], sem.at[i])

    def issue_wd(nb):
        cols = pl.ds(nb * COLS if isinstance(nb, int) else pl.multiple_of(nb * COLS, COLS), COLS)
        for s in range(SB):
            i = slot(Q_WD + nb, s)
            if s < 3:
                put(wd.at[pl.ds(s * ROWS, ROWS), cols], ring.at[i], sem.at[i])
            else:
                put(wd.at[pl.ds(s * ROWS, FF - 3 * ROWS), cols], ring.at[i, pl.ds(0, FF - 3 * ROWS), :], sem.at[i])

    def issue(quad):
        if quad < Q_K0:
            issue_wq(quad)
        elif quad == Q_K0:
            issue_kv(k_hbm, 0, quad)
        elif quad < Q_VL:
            g = (quad - Q_KV) // 2
            if (quad - Q_KV) % 2 == 0:
                issue_kv(k_hbm, g + 1, quad)
            else:
                issue_kv(v_hbm, g, quad)
        elif quad == Q_VL:
            issue_kv(v_hbm, GROUPS - 1, quad)
        elif quad < Q_GU:
            issue_wo(quad - Q_WO)
        elif quad < Q_WD:
            n = quad - Q_GU
            issue_gu(wg if n % 2 == 0 else wu, n // 2, quad)
        elif quad < Q_WD + NB:
            issue_wd(quad - Q_WD)

    def arrive(quad, s, rows=ROWS):
        i = slot(quad, s)
        pltpu.make_async_copy(wq.at[pl.ds(0, rows), pl.ds(0, COLS)], ring.at[i, pl.ds(0, rows), :], sem.at[i]).wait()

    xcopies = [pltpu.make_async_copy(x_hbm.at[:, pl.ds(j * TILE, TILE)], xb.at[j], xsem.at[j]) for j in range(NT)]
    small = [pltpu.make_async_copy(a, b, gsem.at[n]) for n, (a, b) in enumerate(
        ((ga_hbm, gb.at[0]), (gm_hbm, gb.at[1]), (rot_hbm, rb)))]
    for c in xcopies + small:
        c.start()
    for quad in range(R):
        issue(quad)

    barrier = pltpu.get_barrier_semaphore()
    for peer in (sib, far):
        pl.semaphore_signal(barrier, inc=1, device_id={"tp": peer}, device_id_type=pl.DeviceIdType.MESH)

    for c in xcopies + small:
        c.wait()

    def normed(src, gain):
        total = jnp.zeros((BATCH, 128), F32)
        for j in range(NT):
            t = src(j).astype(F32)
            t = t * t
            total += t[:, :128] + t[:, 128:]
        scale = lax.rsqrt(jnp.sum(total, -1, keepdims=True) * (1.0 / D) + 1e-6)
        g = gb[gain].astype(F32)
        for j in range(NT):
            t = src(j).astype(F32)
            row = jnp.concatenate([g[2 * j:2 * j + 1], g[2 * j + 1:2 * j + 2]], 1)
            ab[j] = (t * scale * row).astype(BF16)

    def lhs(kc):
        return jnp.concatenate([ab[kc * 4 + t] for t in range(4)], 1)

    def dot(a, b):
        return jnp.dot(a, b, preferred_element_type=F32)

    normed(lambda j: xb[j], 0)

    cos, sin = rb[0:1, :], rb[1:2, :]
    for nc in range(2):
        for s in range(SB):
            arrive(nc, s)
        for n in range(2):
            acc = None
            for kc in range(4):
                d = dot(lhs(kc), ring[slot(nc, kc), :, n * TILE:(n + 1) * TILE])
                acc = d if acc is None else acc + d
            for hh in range(2):
                t = acc[:, hh * HEAD:(hh + 1) * HEAD].astype(BF16).astype(F32)
                r = t * cos + pltpu.roll(t, HEAD // 2, 1) * sin
                head = nc * 4 + n * 2 + hh
                qb[head * BATCH:(head + 1) * BATCH, :] = r.astype(BF16).astype(F32)
        issue(R + nc)

    row = lax.broadcasted_iota(jnp.int32, (8, 128), 0)
    lane = lax.broadcasted_iota(jnp.int32, (8, 128), 1)
    mine = (lane % 2) == (row // 4)
    zero = jnp.zeros((8, HEAD), F32)
    rate = HEAD**-0.5 * float(np.log2(np.e))

    def scores(g, quad, sc):
        for s in range(SB):
            q = qb[pl.ds(g * SB + s, 8, stride=BATCH), :]
            qq = jnp.concatenate([jnp.concatenate([q, zero], 1), jnp.concatenate([zero, q], 1)], 0).astype(BF16)
            i = slot(quad, s)
            for h in range(2):
                sc[s, h] = lax.dot_general(qq, ring[i, :, h * TILE:(h + 1) * TILE], (((1,), (1,)), ((), ())),
                                           preferred_element_type=F32)

    def attend(g, quad, sc):
        for s in range(SB):
            i = slot(quad, s)
            p = {}
            top = None
            for h in range(2):
                for r in range(2):
                    for c in range(ROWS // 128):
                        t = jnp.where(mine, sc[s, h, r * 8:(r + 1) * 8, c * 128:(c + 1) * 128], NEG)
                        p[h, r, c] = t
                        top = t if top is None else jnp.maximum(top, t)
            top = jnp.max(top, -1, keepdims=True)
            total = None
            for key, t in p.items():
                e = jnp.exp2((t - top) * rate)
                p[key] = e
                total = e if total is None else total + e
            inv = 1.0 / jnp.sum(total, -1, keepdims=True)
            o = None
            for h in range(2):
                w = jnp.concatenate([jnp.concatenate([p[h, r, c] * inv for c in range(ROWS // 128)], 1)
                                     for r in range(2)], 0).astype(BF16)
                d = dot(w, ring[i, :, h * TILE:(h + 1) * TILE])
                o = d if o is None else o + d
            o = o[0:8, 0:HEAD] + o[8:16, HEAD:TILE]
            seen[pl.ds(g * SB + s, 8, stride=BATCH), :] = o.astype(BF16).astype(F32)

    for s in range(SB):
        arrive(Q_K0, s)
    scores(0, Q_K0, sca)
    issue(R + Q_K0)

    def half(g, read, write):
        kq, vq = Q_KV + 2 * g, Q_KV + 1 + 2 * g
        for s in range(SB):
            arrive(kq, s)
            arrive(vq, s)
        scores(g + 1, kq, write)
        attend(g, vq, read)

    def pair(gp, _):
        for e, (read, write) in enumerate(((sca, scb), (scb, sca))):
            g = 2 * gp + e
            half(g, read, write)
            last = (Q_VL - R - Q_KV) // 2

            @pl.when(g < last)
            def _():
                issue_kv(k_hbm, g + 1 + R // 2, Q_KV + 2 * g + R)
                issue_kv(v_hbm, g + R // 2, Q_KV + 1 + 2 * g + R)

            for n in range(last, GROUPS - 2):
                if n % 2 == e:
                    @pl.when(g == n)
                    def _(n=n):
                        issue(Q_KV + 2 * n + R)
                        issue(Q_KV + 1 + 2 * n + R)
        return 0

    lax.fori_loop(0, GROUPS // 2 - 1, pair, 0)
    half(GROUPS - 2, sca, scb)
    issue(Q_KV + 2 * (GROUPS - 2) + R)
    issue(Q_KV + 1 + 2 * (GROUPS - 2) + R)
    for s in range(SB):
        arrive(Q_VL, s)
    attend(GROUPS - 1, Q_VL, scb)
    issue(Q_VL + R)

    def remote(src, dst, a, b, peer):
        return pltpu.make_async_remote_copy(src_ref=src, dst_ref=dst, send_sem=a, recv_sem=b, device_id={"tp": peer},
                                            device_id_type=pl.DeviceIdType.MESH)

    def copy1(e, c):
        return remote(s1.at[e, c, 1 - k], r1.at[e, c], ss1.at[e, c], rs1.at[e, c], sib)

    def copy2(e, c):
        return remote(s2.at[e, c], r2.at[e, c], ss2.at[e, c], rs2.at[e, c], far)

    def copy3(e, c):
        return remote(y.at[e, 2 * c + k], y.at[e, 2 * c + k], ss3.at[e, c], rs3.at[e, c], sib)

    def write(c, which):
        j = 2 * c + which
        cols = pl.ds(pl.multiple_of(j * TILE, TILE), TILE)
        return pltpu.make_async_copy(y.at[1, j], out.at[:, cols], osem.at[j])

    def stage1(e, c, tiles):
        for n in range(2):
            f1[c, n] = tiles[n]
            s1[e, c, n] = tiles[n].astype(BF16)
        copy1(e, c).start()

    def stage2(e, c):
        copy1(e, c).wait_recv()
        s2[e, c] = (f1[c, k] + r1[e, c].astype(F32)).astype(BF16)
        copy2(e, c).start()

    def stage3(e, c):
        copy2(e, c).wait_recv()
        j = 2 * c + k
        base = (xb[j] if e == 0 else y[0, j]).astype(F32)
        y[e, j] = (base + (s2[e, c].astype(F32) + r2[e, c].astype(F32))).astype(BF16)
        copy3(e, c).start()
        if e == 1:
            write(c, k).start()

    def stage4(e, c):
        copy3(e, c).wait_recv()
        if e == 1:
            write(c, 1 - k).start()

    def behind(e, c):
        @pl.when(c >= 1)
        def _():
            stage2(e, c - 1)

        @pl.when(c >= 3)
        def _():
            stage3(e, c - 3)

    def drain(e):
        stage2(e, NB - 1)
        for c in range(NB - 3, NB):
            stage3(e, c)
        for c in range(NB):
            stage4(e, c)

    def sent(e):
        for c in range(NB):
            copy1(e, c).wait_send()
            copy2(e, c).wait_send()
            copy3(e, c).wait_send()

    pl.semaphore_wait(barrier, 2)

    def wo_step(c, _):
        arrive(Q_WO + c // SB, lax.rem(c, SB))
        i = slot(Q_WO + c // SB, lax.rem(c, SB))
        a = jnp.concatenate([seen[h * BATCH:(h + 1) * BATCH, :].astype(BF16) for h in range(8)], 1)
        stage1(0, c, [dot(a, ring[i, :, n * TILE:(n + 1) * TILE]) for n in range(2)])
        behind(0, c)
        return 0

    lax.fori_loop(0, NB, wo_step, 0)
    issue(Q_WO + R)
    issue(Q_WO + 1 + R)
    drain(0)
    normed(lambda j: y[0, j], 1)

    def gu_step(nb, _):
        gq, uq = Q_GU + 2 * nb, Q_GU + 1 + 2 * nb
        for s in range(SB):
            arrive(gq, s)
            arrive(uq, s)
        for n in range(2):
            cols = slice(n * TILE, (n + 1) * TILE)
            gate = up = None
            for kc in range(4):
                d = dot(lhs(kc), ring[slot(gq, kc), :, cols])
                gate = d if gate is None else gate + d
            for kc in range(4):
                d = dot(lhs(kc), ring[slot(uq, kc), :, cols])
                up = d if up is None else up + d
            hid[nb, :, cols] = (jax.nn.silu(gate) * up).astype(BF16)
        for n in range(NF):
            if Q_GU + 2 * n + R < Q_WD + NB:
                @pl.when(nb == n)
                def _(n=n):
                    issue(Q_GU + 2 * n + R)
                    issue(Q_GU + 1 + 2 * n + R)
        return 0

    lax.fori_loop(0, NF, gu_step, 0)

    def wd_step(c, _):
        for s in range(3):
            arrive(Q_WD + c, s)
        arrive(Q_WD + c, 3, FF - 3 * ROWS)
        tiles = []
        for n in range(2):
            cols = slice(n * TILE, (n + 1) * TILE)
            acc = None
            for kc in range(4):
                i = slot(Q_WD + c, kc)
                if kc < 3:
                    d = dot(jnp.concatenate([hid[2 * kc], hid[2 * kc + 1]], 1), ring[i, :, cols])
                else:
                    d = dot(hid[NF - 1], ring[i, 0:FF - 3 * ROWS, cols])
                acc = d if acc is None else acc + d
            tiles.append(acc)
        stage1(1, c, tiles)
        behind(1, c)
        return 0

    lax.fori_loop(0, NB, wd_step, 0)
    drain(1)
    sent(0)
    sent(1)
    for c in range(NB):
        for n in range(2):
            write(c, n).wait()


def solution(mesh):
    half = HEAD // 2
    angle = (CACHE - 1) * float(THETA) ** (-np.arange(half) / half)
    turn = np.zeros((8, HEAD), np.float32)
    turn[0] = np.concatenate([np.cos(angle), np.cos(angle)])
    turn[1] = np.concatenate([-np.sin(angle), np.sin(angle)])
    hbm = pl.BlockSpec(memory_space=pl.ANY)

    def step(x, k_cache, v_cache, gain_a, wq, wo, gain_m, w_gate, w_up, w_down):
        flat = (BATCH, CACHE * KV, HEAD)
        dma = pltpu.SemaphoreType.DMA
        call = pl.pallas_call(
            kernel,
            out_shape=jax.ShapeDtypeStruct((BATCH, D), BF16),
            in_specs=[hbm] * 11,
            out_specs=hbm,
            scratch_shapes=[
                pltpu.VMEM((R * SB, ROWS, COLS), BF16),
                pltpu.VMEM((NT, BATCH, TILE), BF16),
                pltpu.VMEM((NT, BATCH, TILE), BF16),
                pltpu.VMEM((2, D // 128, 128), BF16),
                pltpu.VMEM((8, HEAD), F32),
                pltpu.VMEM((8 * BATCH, HEAD), F32),
                pltpu.VMEM((SB, 2, 16, ROWS), F32),
                pltpu.VMEM((SB, 2, 16, ROWS), F32),
                pltpu.VMEM((8 * BATCH, HEAD), F32),
                pltpu.VMEM((NF, BATCH, COLS), BF16),
                pltpu.VMEM((NB, 2, BATCH, TILE), F32),
                pltpu.VMEM((2, NB, 2, BATCH, TILE), BF16),
                pltpu.VMEM((2, NB, BATCH, TILE), BF16),
                pltpu.VMEM((2, NB, BATCH, TILE), BF16),
                pltpu.VMEM((2, NB, BATCH, TILE), BF16),
                pltpu.VMEM((2, NT, BATCH, TILE), BF16),
                dma((R * SB,)), dma((NT,)), dma((3,)),
                dma((2, NB)), dma((2, NB)), dma((2, NB)), dma((2, NB)), dma((2, NB)), dma((2, NB)), dma((NT,)),
            ],
            compiler_params=pltpu.CompilerParams(collective_id=0, has_side_effects=True, vmem_limit_bytes=67_000_000),
            cost_estimate=pl.CostEstimate(flops=20 * 10**9, bytes_accessed=240 * 10**6, transcendentals=0),
            name="layer",
        )
        return call(x, k_cache.reshape(flat), v_cache.reshape(flat), gain_a.reshape(D // 128, 128), wq, wo,
                    gain_m.reshape(D // 128, 128), w_gate, w_up, w_down, jnp.asarray(turn))

    states, cache, columns, rows_of = P("dp", None), P("dp", None, "tp", None), P(None, "tp"), P("tp", None)
    return jax.shard_map(
        step,
        mesh=mesh,
        in_specs=(states, cache, cache, P(None), columns, rows_of, P(None), columns, columns, rows_of),
        out_specs=states,
        check_vma=False,
    )
```

```python
import jax
import jax.numpy as jnp
import numpy as np
from jax import lax
from jax.experimental import pallas as pl
from jax.experimental.pallas import tpu as pltpu
from jax.sharding import PartitionSpec as P

HEAD = 128
THETA = 10000
BATCH = 64
CACHE = 2048
KV = 2
D = 4096
FF = 3584
ROWS, COLS = 1024, 512
SB = 4
R = 11
HALF = BATCH // 2
GROUPS = BATCH // SB
TILE = 256
NT = D // TILE
NB = D // COLS
NF = FF // COLS
Q_K0, Q_KV, Q_VL, Q_GU, Q_WD = 0, 1, 31, 32, 46
F32, BF16 = jnp.float32, jnp.bfloat16
NEG = float("-inf")


def kernel(x_hbm, k_hbm, v_hbm, ga_hbm, wq, wo, gm_hbm, wg, wu, wd, rot_hbm, out,
           ring, held, xb, ab, gb, rb, qb, sca, scb, seen, hid, f1, s1, r1, s2, r2, y,
           sem, wsem, xsem, gsem, ss1, rs1, ss2, rs2, ss3, rs3):
    tp = lax.axis_index("tp")
    k = lax.rem(tp, 2)
    sib = tp + 1 - 2 * k
    far = lax.rem(tp + 2, 4)

    def slot(quad, s):
        return (quad % R if isinstance(quad, int) else lax.rem(quad, R)) * SB + s

    def put(src, dst, s):
        pltpu.make_async_copy(src, dst, s).start(priority=1)

    def issue_wq():
        for i in range(2 * SB):
            pltpu.make_async_copy(wq.at[pl.ds(i % SB * ROWS, ROWS), pl.ds(i // SB * COLS, COLS)], held.at[i], wsem.at[i]).start()

    def issue_kv(ref, g, quad):
        for s in range(SB):
            i = slot(quad, s)
            for c in range(4):
                put(ref.at[g * SB + s, pl.ds(c * ROWS, ROWS), :], ring.at[i, :, pl.ds(c * 128, 128)], sem.at[i])

    def issue_wo():
        for i in range(NB):
            put(wo.at[:, pl.ds(i * COLS, COLS)], held.at[i], wsem.at[i])

    def issue_gu(ref, nb, quad):
        for s in range(SB):
            i = slot(quad, s)
            cols = pl.ds(nb * COLS if isinstance(nb, int) else pl.multiple_of(nb * COLS, COLS), COLS)
            put(ref.at[pl.ds(s * ROWS, ROWS), cols], ring.at[i], sem.at[i])

    def issue_wd(nb):
        cols = pl.ds(nb * COLS if isinstance(nb, int) else pl.multiple_of(nb * COLS, COLS), COLS)
        for s in range(SB):
            i = slot(Q_WD + nb, s)
            if s < 3:
                put(wd.at[pl.ds(s * ROWS, ROWS), cols], ring.at[i], sem.at[i])
            else:
                put(wd.at[pl.ds(s * ROWS, FF - 3 * ROWS), cols], ring.at[i, pl.ds(0, FF - 3 * ROWS), :], sem.at[i])

    def issue(quad):
        if quad == Q_K0:
            issue_kv(k_hbm, 0, quad)
        elif quad < Q_VL:
            g = (quad - Q_KV) // 2
            if (quad - Q_KV) % 2 == 0:
                issue_kv(k_hbm, g + 1, quad)
            else:
                issue_kv(v_hbm, g, quad)
        elif quad == Q_VL:
            issue_kv(v_hbm, GROUPS - 1, quad)
        elif quad < Q_WD:
            n = quad - Q_GU
            issue_gu(wg if n % 2 == 0 else wu, n // 2, quad)
        elif quad < Q_WD + NB:
            issue_wd(quad - Q_WD)

    def arrive(quad, s, rows=ROWS):
        i = slot(quad, s)
        pltpu.make_async_copy(wq.at[pl.ds(0, rows), pl.ds(0, COLS)], ring.at[i, pl.ds(0, rows), :], sem.at[i]).wait()

    def held_arrive(i):
        pltpu.make_async_copy(wq.at[pl.ds(0, ROWS), pl.ds(0, COLS)], held.at[i], wsem.at[i]).wait()

    xcopies = [pltpu.make_async_copy(x_hbm.at[:, pl.ds(j * TILE, TILE)], xb.at[j], xsem.at[j]) for j in range(NT)]
    small = [pltpu.make_async_copy(a, b, gsem.at[n]) for n, (a, b) in enumerate(
        ((ga_hbm, gb.at[0]), (gm_hbm, gb.at[1]), (rot_hbm, rb)))]
    for c in xcopies + small:
        c.start()
    issue_wq()
    for quad in range(R):
        issue(quad)

    barrier = pltpu.get_barrier_semaphore()
    for peer in (sib, far):
        pl.semaphore_signal(barrier, inc=1, device_id={"tp": peer}, device_id_type=pl.DeviceIdType.MESH)

    for c in xcopies + small:
        c.wait()

    def normed(src, gain):
        total = jnp.zeros((BATCH, 128), F32)
        for j in range(NT):
            t = src(j).astype(F32)
            t = t * t
            total += t[:, :128] + t[:, 128:]
        scale = lax.rsqrt(jnp.sum(total, -1, keepdims=True) * (1.0 / D) + 1e-6)
        g = gb[gain].astype(F32)
        for j in range(NT):
            t = src(j).astype(F32)
            row = jnp.concatenate([g[2 * j:2 * j + 1], g[2 * j + 1:2 * j + 2]], 1)
            ab[j] = (t * scale * row).astype(BF16)

    def lhs(kc):
        return jnp.concatenate([ab[kc * 4 + t] for t in range(4)], 1)

    def dot(a, b):
        return jnp.dot(a, b, preferred_element_type=F32)

    normed(lambda j: xb[j], 0)

    cos, sin = rb[0:1, :], rb[1:2, :]
    for nc in range(2):
        for s in range(SB):
            held_arrive(nc * SB + s)
        for n in range(2):
            acc = None
            for kc in range(4):
                d = dot(lhs(kc), held[nc * SB + kc, :, n * TILE:(n + 1) * TILE])
                acc = d if acc is None else acc + d
            for hh in range(2):
                t = acc[:, hh * HEAD:(hh + 1) * HEAD].astype(BF16).astype(F32)
                r = t * cos + pltpu.roll(t, HEAD // 2, 1) * sin
                head = nc * 4 + n * 2 + hh
                qb[head * BATCH:(head + 1) * BATCH, :] = r.astype(BF16).astype(F32)
    issue_wo()

    row = lax.broadcasted_iota(jnp.int32, (8, 128), 0)
    lane = lax.broadcasted_iota(jnp.int32, (8, 128), 1)
    mine = (lane % 2) == (row // 4)
    zero = jnp.zeros((8, HEAD), F32)
    rate = HEAD**-0.5 * float(np.log2(np.e))

    def scores(g, quad, sc):
        for s in range(SB):
            q = qb[pl.ds(g * SB + s, 8, stride=BATCH), :]
            qq = jnp.concatenate([jnp.concatenate([q, zero], 1), jnp.concatenate([zero, q], 1)], 0).astype(BF16)
            i = slot(quad, s)
            for h in range(2):
                sc[s, h] = lax.dot_general(qq, ring[i, :, h * TILE:(h + 1) * TILE], (((1,), (1,)), ((), ())),
                                           preferred_element_type=F32)

    def attend(g, quad, sc):
        for s in range(SB):
            i = slot(quad, s)
            p = {}
            top = None
            for h in range(2):
                for r in range(2):
                    for c in range(ROWS // 128):
                        t = jnp.where(mine, sc[s, h, r * 8:(r + 1) * 8, c * 128:(c + 1) * 128], NEG)
                        p[h, r, c] = t
                        top = t if top is None else jnp.maximum(top, t)
            top = jnp.max(top, -1, keepdims=True)
            total = None
            for key, t in p.items():
                e = jnp.exp2((t - top) * rate)
                p[key] = e
                total = e if total is None else total + e
            inv = 1.0 / jnp.sum(total, -1, keepdims=True)
            o = None
            for h in range(2):
                w = jnp.concatenate([jnp.concatenate([p[h, r, c] * inv for c in range(ROWS // 128)], 1)
                                     for r in range(2)], 0).astype(BF16)
                d = dot(w, ring[i, :, h * TILE:(h + 1) * TILE])
                o = d if o is None else o + d
            o = o[0:8, 0:HEAD] + o[8:16, HEAD:TILE]
            seen[pl.ds(g * SB + s, 8, stride=BATCH), :] = o.astype(BF16).astype(F32)

    def rows(e):
        return pl.ds(0, BATCH if e == 2 else HALF)

    def place(e):
        return (1, pl.ds(0, BATCH)) if e == 2 else (0, pl.ds(e * HALF, HALF))
    def remote(src, dst, a, b, peer):
        return pltpu.make_async_remote_copy(src_ref=src, dst_ref=dst, send_sem=a, recv_sem=b, device_id={"tp": peer},
                                            device_id_type=pl.DeviceIdType.MESH)

    def copy1(e, c):
        return remote(s1.at[e, c, 1 - k, rows(e)], r1.at[e, c, rows(e)], ss1.at[e, c], rs1.at[e, c], sib)

    def copy2(e, c):
        return remote(s2.at[e, c, rows(e)], r2.at[e, c, rows(e)], ss2.at[e, c], rs2.at[e, c], far)

    def copy3(e, c):
        which, at = place(e)
        return remote(y.at[which, 2 * c + k, at], y.at[which, 2 * c + k, at], ss3.at[e, c], rs3.at[e, c], sib)

    def stage1(e, c, tiles):
        for n in range(2):
            f1[c, n, rows(e)] = tiles[n]
            s1[e, c, n, rows(e)] = tiles[n].astype(BF16)
        copy1(e, c).start()

    def stage2(e, c):
        copy1(e, c).wait_recv()
        s2[e, c, rows(e)] = (f1[c, k, rows(e)] + r1[e, c, rows(e)].astype(F32)).astype(BF16)
        copy2(e, c).start()

    def stage3(e, c):
        copy2(e, c).wait_recv()
        j = 2 * c + k
        which, at = place(e)
        base = (y[0, j] if e == 2 else xb[j, at]).astype(F32)
        y[which, j, at] = (base + (s2[e, c, rows(e)].astype(F32) + r2[e, c, rows(e)].astype(F32))).astype(BF16)
        copy3(e, c).start()

    def stage4(e, c):
        copy3(e, c).wait_recv()
        if e == 2:
            for j in (2 * c, 2 * c + 1):
                out[:, j * TILE:(j + 1) * TILE] = y[1, j]

    def behind(e, c):
        @pl.when(c >= 2)
        def _():
            stage2(e, c - 2)

        @pl.when(c >= 5)
        def _():
            stage3(e, c - 5)

    def drain(e):
        for c in range(NB - 2, NB):
            stage2(e, c)
        for c in range(NB - 5, NB):
            stage3(e, c)
        for c in range(NB):
            stage4(e, c)

    def sent(e):
        for c in range(NB):
            copy1(e, c).wait_send()
            copy2(e, c).wait_send()
            copy3(e, c).wait_send()

    def loop(body):
        def one(c, _):
            body(c)
            return 0
        lax.fori_loop(0, NB, one, 0)

    def wo_steps(e):
        def one(c):
            at = e * HALF
            a = jnp.concatenate([seen[h * BATCH + at:h * BATCH + at + HALF, :].astype(BF16) for h in range(8)], 1)
            stage1(e, c, [dot(a, held[c, :, n * TILE:(n + 1) * TILE]) for n in range(2)])
        loop(one)

    for s in range(SB):
        arrive(Q_K0, s)
    scores(0, Q_K0, sca)
    issue(R + Q_K0)

    def half(g, read, write):
        kq, vq = Q_KV + 2 * g, Q_KV + 1 + 2 * g
        for s in range(SB):
            arrive(kq, s)
            arrive(vq, s)
        scores(g + 1, kq, write)
        attend(g, vq, read)

    def pair(gp, _):
        for e, (read, write) in enumerate(((sca, scb), (scb, sca))):
            g = 2 * gp + e
            half(g, read, write)
            last = (Q_VL - R - Q_KV) // 2

            @pl.when(g < last)
            def _():
                if R % 2 == 0:
                    issue_kv(k_hbm, g + 1 + R // 2, Q_KV + 2 * g + R)
                    issue_kv(v_hbm, g + R // 2, Q_KV + 1 + 2 * g + R)
                else:
                    issue_kv(v_hbm, g + R // 2, Q_KV + 2 * g + R)
                    issue_kv(k_hbm, g + 2 + R // 2, Q_KV + 1 + 2 * g + R)

            for n in range(last, GROUPS - 2):
                if n % 2 == e:
                    @pl.when(g == n)
                    def _(n=n):
                        issue(Q_KV + 2 * n + R)
                        issue(Q_KV + 1 + 2 * n + R)

        @pl.when(gp == GROUPS // 4 - 1)
        def _():
            pl.semaphore_wait(barrier, 2)
            for i in range(NB):
                held_arrive(i)
            wo_steps(0)

        @pl.when(gp == GROUPS // 4)
        def _():
            loop(lambda c: stage2(0, c))

        @pl.when(gp == GROUPS // 4 + 1)
        def _():
            loop(lambda c: stage3(0, c))
        return 0

    lax.fori_loop(0, GROUPS // 2 - 1, pair, 0)
    half(GROUPS - 2, sca, scb)
    issue(Q_KV + 2 * (GROUPS - 2) + R)
    issue(Q_KV + 1 + 2 * (GROUPS - 2) + R)
    for s in range(SB):
        arrive(Q_VL, s)
    attend(GROUPS - 1, Q_VL, scb)
    issue(Q_VL + R)

    wo_steps(1)
    loop(lambda c: stage2(1, c))
    loop(lambda c: stage3(1, c))
    for e in range(2):
        for c in range(NB):
            stage4(e, c)
    normed(lambda j: y[0, j], 1)

    def gu_step(nb, _):
        gq, uq = Q_GU + 2 * nb, Q_GU + 1 + 2 * nb
        for s in range(SB):
            arrive(gq, s)
            arrive(uq, s)
        for n in range(2):
            cols = slice(n * TILE, (n + 1) * TILE)
            gate = up = None
            for kc in range(4):
                d = dot(lhs(kc), ring[slot(gq, kc), :, cols])
                gate = d if gate is None else gate + d
            for kc in range(4):
                d = dot(lhs(kc), ring[slot(uq, kc), :, cols])
                up = d if up is None else up + d
            hid[nb, :, cols] = (jax.nn.silu(gate) * up).astype(BF16)
        for n in range(NF):
            if Q_GU + 2 * n + R < Q_WD + NB:
                @pl.when(nb == n)
                def _(n=n):
                    issue(Q_GU + 2 * n + R)
                    issue(Q_GU + 1 + 2 * n + R)
        return 0

    lax.fori_loop(0, NF, gu_step, 0)

    def wd_step(c, _):
        for s in range(3):
            arrive(Q_WD + c, s)
        arrive(Q_WD + c, 3, FF - 3 * ROWS)
        tiles = []
        for n in range(2):
            cols = slice(n * TILE, (n + 1) * TILE)
            acc = None
            for kc in range(4):
                i = slot(Q_WD + c, kc)
                if kc < 3:
                    d = dot(jnp.concatenate([hid[2 * kc], hid[2 * kc + 1]], 1), ring[i, :, cols])
                else:
                    d = dot(hid[NF - 1], ring[i, 0:FF - 3 * ROWS, cols])
                acc = d if acc is None else acc + d
            tiles.append(acc)
        stage1(2, c, tiles)
        behind(2, c)
        return 0

    sent(0)
    sent(1)
    lax.fori_loop(0, NB, wd_step, 0)
    drain(2)
    sent(2)


def solution(mesh):
    half = HEAD // 2
    angle = (CACHE - 1) * float(THETA) ** (-np.arange(half) / half)
    turn = np.zeros((8, HEAD), np.float32)
    turn[0] = np.concatenate([np.cos(angle), np.cos(angle)])
    turn[1] = np.concatenate([-np.sin(angle), np.sin(angle)])
    hbm = pl.BlockSpec(memory_space=pl.ANY)

    def step(x, k_cache, v_cache, gain_a, wq, wo, gain_m, w_gate, w_up, w_down):
        flat = (BATCH, CACHE * KV, HEAD)
        dma = pltpu.SemaphoreType.DMA
        call = pl.pallas_call(
            kernel,
            out_shape=pltpu.VMEM((BATCH, D), BF16),
            in_specs=[hbm] * 11,
            out_specs=pl.BlockSpec(memory_space=pltpu.VMEM),
            scratch_shapes=[
                pltpu.VMEM((R * SB, ROWS, COLS), BF16),
                pltpu.VMEM((NB, ROWS, COLS), BF16),
                pltpu.VMEM((NT, BATCH, TILE), BF16),
                pltpu.VMEM((NT, BATCH, TILE), BF16),
                pltpu.VMEM((2, D // 128, 128), BF16),
                pltpu.VMEM((8, HEAD), F32),
                pltpu.VMEM((8 * BATCH, HEAD), F32),
                pltpu.VMEM((SB, 2, 16, ROWS), F32),
                pltpu.VMEM((SB, 2, 16, ROWS), F32),
                pltpu.VMEM((8 * BATCH, HEAD), F32),
                pltpu.VMEM((NF, BATCH, COLS), BF16),
                pltpu.VMEM((NB, 2, BATCH, TILE), F32),
                pltpu.VMEM((3, NB, 2, BATCH, TILE), BF16),
                pltpu.VMEM((3, NB, BATCH, TILE), BF16),
                pltpu.VMEM((3, NB, BATCH, TILE), BF16),
                pltpu.VMEM((3, NB, BATCH, TILE), BF16),
                pltpu.VMEM((2, NT, BATCH, TILE), BF16),
                dma((R * SB,)), dma((NB,)), dma((NT,)), dma((3,)),
                *[dma((3, NB))] * 6,
            ],
            compiler_params=pltpu.CompilerParams(collective_id=0, has_side_effects=True, vmem_limit_bytes=65_900_000),
            cost_estimate=pl.CostEstimate(flops=20 * 10**9, bytes_accessed=240 * 10**6, transcendentals=0),
            name="layer",
        )
        return call(x, k_cache.reshape(flat), v_cache.reshape(flat), gain_a.reshape(D // 128, 128), wq, wo,
                    gain_m.reshape(D // 128, 128), w_gate, w_up, w_down, jnp.asarray(turn))

    states, cache, columns, rows_of = P("dp", None), P("dp", None, "tp", None), P(None, "tp"), P("tp", None)
    return jax.shard_map(
        step,
        mesh=mesh,
        in_specs=(states, cache, cache, P(None), columns, rows_of, P(None), columns, columns, rows_of),
        out_specs=states,
        check_vma=False,
    )
```

```python
import jax
import jax.numpy as jnp
import numpy as np
from jax import lax
from jax.experimental import pallas as pl
from jax.experimental.pallas import tpu as pltpu
from jax.sharding import PartitionSpec as P

HEAD = 128
THETA = 10000
BATCH = 64
CACHE = 2048
KV = 2
D = 4096
FF = 3584
ROWS, COLS = 1024, 512
SB = 4
R = 11
EARLY = 48
GROUPS = BATCH // SB
TILE = 256
NT = D // TILE
NB = D // COLS
NF = FF // COLS
Q_K0, Q_KV, Q_VL, Q_GU, Q_WD = 0, 1, 31, 32, 46
F32, BF16 = jnp.float32, jnp.bfloat16
NEG = float("-inf")


def kernel(x_hbm, k_hbm, v_hbm, ga_hbm, wq, wo, gm_hbm, wg, wu, wd, rot_hbm, out,
           ring, held, xb, ab, gb, rb, qb, sca, scb, seen, hid, f1, s1, r1, s2, r2, y,
           fz, sz, rz, yz, sem, wsem, lsem, xsem, gsem, xs, xr):
    tp = lax.axis_index("tp")
    k = lax.rem(tp, 2)
    sib = tp + 1 - 2 * k
    far = lax.rem(tp + 2, 4)

    def slot(quad, s):
        return (quad % R if isinstance(quad, int) else lax.rem(quad, R)) * SB + s

    def put(src, dst, s):
        pltpu.make_async_copy(src, dst, s).start(priority=1)

    def issue_wq():
        for i in range(2 * SB):
            pltpu.make_async_copy(wq.at[pl.ds(i % SB * ROWS, ROWS), pl.ds(i // SB * COLS, COLS)], held.at[i], wsem.at[i]).start()

    def issue_kv(ref, g, quad):
        for s in range(SB):
            i = slot(quad, s)
            for c in range(4):
                put(ref.at[g * SB + s, pl.ds(c * ROWS, ROWS), :], ring.at[i, :, pl.ds(c * 128, 128)], sem.at[i])

    def issue_wo():
        for i in range(NB):
            put(wo.at[:, pl.ds(i * COLS, COLS)], held.at[i], wsem.at[i])

    def issue_gu(ref, nb, quad):
        for s in range(SB):
            i = slot(quad, s)
            cols = pl.ds(nb * COLS if isinstance(nb, int) else pl.multiple_of(nb * COLS, COLS), COLS)
            put(ref.at[pl.ds(s * ROWS, ROWS), cols], ring.at[i], sem.at[i])

    def issue_last():
        for n in range(2):
            for s in range(SB):
                rows = ROWS if s < 3 else FF - 3 * ROWS
                put(wd.at[pl.ds(s * ROWS, rows), pl.ds((NT - 2 + n) * TILE, TILE)],
                    ring.at[slot(Q_WD + NB - 1, s), pl.ds(0, rows), pl.ds(n * TILE, TILE)], lsem.at[n, s])

    def last_arrive(n):
        for s in range(SB):
            rows = ROWS if s < 3 else FF - 3 * ROWS
            pltpu.make_async_copy(wd.at[pl.ds(0, rows), pl.ds(0, TILE)],
                                  ring.at[slot(Q_WD + NB - 1, s), pl.ds(0, rows), pl.ds(n * TILE, TILE)], lsem.at[n, s]).wait()

    def issue_wd(nb):
        cols = pl.ds(nb * COLS if isinstance(nb, int) else pl.multiple_of(nb * COLS, COLS), COLS)
        for s in range(SB):
            i = slot(Q_WD + nb, s)
            if s < 3:
                put(wd.at[pl.ds(s * ROWS, ROWS), cols], ring.at[i], sem.at[i])
            else:
                put(wd.at[pl.ds(s * ROWS, FF - 3 * ROWS), cols], ring.at[i, pl.ds(0, FF - 3 * ROWS), :], sem.at[i])

    def issue(quad):
        if quad == Q_K0:
            issue_kv(k_hbm, 0, quad)
        elif quad < Q_VL:
            g = (quad - Q_KV) // 2
            if (quad - Q_KV) % 2 == 0:
                issue_kv(k_hbm, g + 1, quad)
            else:
                issue_kv(v_hbm, g, quad)
        elif quad == Q_VL:
            issue_kv(v_hbm, GROUPS - 1, quad)
        elif quad < Q_WD:
            n = quad - Q_GU
            issue_gu(wg if n % 2 == 0 else wu, n // 2, quad)
        elif quad < Q_WD + NB - 1:
            issue_wd(quad - Q_WD)
        elif quad == Q_WD + NB - 1:
            issue_last()

    def arrive(quad, s, rows=ROWS):
        i = slot(quad, s)
        pltpu.make_async_copy(wq.at[pl.ds(0, rows), pl.ds(0, COLS)], ring.at[i, pl.ds(0, rows), :], sem.at[i]).wait()

    def held_arrive(i):
        pltpu.make_async_copy(wq.at[pl.ds(0, ROWS), pl.ds(0, COLS)], held.at[i], wsem.at[i]).wait()

    xcopies = [pltpu.make_async_copy(x_hbm.at[:, pl.ds(j * TILE, TILE)], xb.at[j], xsem.at[j]) for j in range(NT)]
    small = [pltpu.make_async_copy(a, b, gsem.at[n]) for n, (a, b) in enumerate(
        ((ga_hbm, gb.at[0]), (gm_hbm, gb.at[1]), (rot_hbm, rb)))]
    for c in xcopies + small:
        c.start()
    issue_wq()
    for quad in range(R):
        issue(quad)

    barrier = pltpu.get_barrier_semaphore()
    for peer in (sib, far):
        pl.semaphore_signal(barrier, inc=1, device_id={"tp": peer}, device_id_type=pl.DeviceIdType.MESH)

    for c in xcopies + small:
        c.wait()

    def normed(src, gain):
        total = jnp.zeros((BATCH, 128), F32)
        for j in range(NT):
            t = src(j).astype(F32)
            t = t * t
            total += t[:, :128] + t[:, 128:]
        scale = lax.rsqrt(jnp.sum(total, -1, keepdims=True) * (1.0 / D) + 1e-6)
        g = gb[gain].astype(F32)
        for j in range(NT):
            t = src(j).astype(F32)
            row = jnp.concatenate([g[2 * j:2 * j + 1], g[2 * j + 1:2 * j + 2]], 1)
            ab[j] = (t * scale * row).astype(BF16)

    def lhs(kc):
        return jnp.concatenate([ab[kc * 4 + t] for t in range(4)], 1)

    def dot(a, b):
        return jnp.dot(a, b, preferred_element_type=F32)

    normed(lambda j: xb[j], 0)

    cos, sin = rb[0:1, :], rb[1:2, :]
    for nc in range(2):
        for s in range(SB):
            held_arrive(nc * SB + s)
        for n in range(2):
            acc = None
            for kc in range(4):
                d = dot(lhs(kc), held[nc * SB + kc, :, n * TILE:(n + 1) * TILE])
                acc = d if acc is None else acc + d
            for hh in range(2):
                t = acc[:, hh * HEAD:(hh + 1) * HEAD].astype(BF16).astype(F32)
                r = t * cos + pltpu.roll(t, HEAD // 2, 1) * sin
                head = nc * 4 + n * 2 + hh
                qb[head * BATCH:(head + 1) * BATCH, :] = r.astype(BF16).astype(F32)
    issue_wo()

    row = lax.broadcasted_iota(jnp.int32, (8, 128), 0)
    lane = lax.broadcasted_iota(jnp.int32, (8, 128), 1)
    mine = (lane % 2) == (row // 4)
    zero = jnp.zeros((8, HEAD), F32)
    rate = HEAD**-0.5 * float(np.log2(np.e))

    def scores(g, quad, sc):
        for s in range(SB):
            q = qb[pl.ds(g * SB + s, 8, stride=BATCH), :]
            qq = jnp.concatenate([jnp.concatenate([q, zero], 1), jnp.concatenate([zero, q], 1)], 0).astype(BF16)
            i = slot(quad, s)
            for h in range(2):
                sc[s, h] = lax.dot_general(qq, ring[i, :, h * TILE:(h + 1) * TILE], (((1,), (1,)), ((), ())),
                                           preferred_element_type=F32)

    def attend(g, quad, sc):
        for s in range(SB):
            i = slot(quad, s)
            p = {}
            top = None
            for h in range(2):
                for r in range(2):
                    for c in range(ROWS // 128):
                        t = jnp.where(mine, sc[s, h, r * 8:(r + 1) * 8, c * 128:(c + 1) * 128], NEG)
                        p[h, r, c] = t
                        top = t if top is None else jnp.maximum(top, t)
            top = jnp.max(top, -1, keepdims=True)
            total = None
            for key, t in p.items():
                e = jnp.exp2((t - top) * rate)
                p[key] = e
                total = e if total is None else total + e
            inv = 1.0 / jnp.sum(total, -1, keepdims=True)
            o = None
            for h in range(2):
                w = jnp.concatenate([jnp.concatenate([p[h, r, c] * inv for c in range(ROWS // 128)], 1)
                                     for r in range(2)], 0).astype(BF16)
                d = dot(w, ring[i, :, h * TILE:(h + 1) * TILE])
                o = d if o is None else o + d
            o = o[0:8, 0:HEAD] + o[8:16, HEAD:TILE]
            seen[pl.ds(g * SB + s, 8, stride=BATCH), :] = o.astype(BF16).astype(F32)

    def remote(src, dst, stage, n, peer):
        return pltpu.make_async_remote_copy(src_ref=src, dst_ref=dst, send_sem=xs.at[stage, n], recv_sem=xr.at[stage, n],
                                            device_id={"tp": peer}, device_id_type=pl.DeviceIdType.MESH)

    class Unit:
        def __init__(self, e, c):
            self.e, self.c = e, c
            if e < 3:
                t = 2 if e < 2 else 1
                at = (pl.ds(0, EARLY), pl.ds(EARLY, BATCH - EARLY), pl.ds(0, BATCH))[e]
                p = e // 2
                own, other, got = pl.ds(2 * t * c + t * k, t), pl.ds(2 * t * c + t * (1 - k), t), pl.ds(t * c, t)
                self.n = (0, NB // 2, NB)[e] + c
                self.term, self.give, self.take = f1.at[own, at], s1.at[p, other, at], r1.at[p, got, at]
                self.pair, self.far = s2.at[p, got, at], r2.at[p, got, at]
                self.base = xb.at[own, at] if e < 2 else y.at[0, own]
                self.result = y.at[p, own, at]
            else:
                self.n = 2 * NB + c
                half = pl.ds(pl.multiple_of(k * 128, 128), 128)
                self.term, self.give, self.take = fz.at[c, k], sz.at[c, 1 - k], rz.at[c, 0]
                self.pair, self.far = rz.at[c, 1], rz.at[c, 2]
                self.base, self.result = y.at[0, NT - 2 + c, :, half], yz.at[c, k]

        def copy1(self):
            return remote(self.give, self.take, 0, self.n, sib)

        def copy2(self):
            return remote(self.pair, self.far, 1, self.n, far)

        def copy3(self):
            return remote(self.result, self.result, 2, self.n, sib)

    def stage1(e, c):
        Unit(e, c).copy1().start()

    def stage2(e, c):
        u = Unit(e, c)
        u.copy1().wait_recv()
        u.pair[...] = (u.term[...] + u.take[...].astype(F32)).astype(BF16)
        u.copy2().start()

    def stage3(e, c):
        u = Unit(e, c)
        u.copy2().wait_recv()
        u.result[...] = (u.base[...].astype(F32) + (u.pair[...].astype(F32) + u.far[...].astype(F32))).astype(BF16)
        u.copy3().start()

    def stage4(e, c):
        Unit(e, c).copy3().wait_recv()
        if e == 2:
            for j in (2 * c, 2 * c + 1):
                out[:, j * TILE:(j + 1) * TILE] = y[1, j]
        elif e == 3:
            for n in range(2):
                out[:, (NT - 2 + c) * TILE + n * 128:(NT - 2 + c) * TILE + (n + 1) * 128] = yz[c, n]

    def sent(e, c):
        u = Unit(e, c)
        u.copy1().wait_send()
        u.copy2().wait_send()
        u.copy3().wait_send()

    def keep(p, j, at, t):
        f1[j, at] = t
        s1[p, j, at] = t.astype(BF16)

    def wo_steps(e):
        at = slice(0, EARLY) if e == 0 else slice(EARLY, BATCH)
        a = jnp.concatenate([seen[h * BATCH + at.start:h * BATCH + at.stop, :].astype(BF16) for h in range(8)], 1)
        for j in range(NT):
            keep(0, j, at, dot(a, held[j // 2, :, j % 2 * TILE:(j % 2 + 1) * TILE]))
            if j % 4 == 3:
                stage1(e, j // 4)

    for s in range(SB):
        arrive(Q_K0, s)
    scores(0, Q_K0, sca)
    issue(R + Q_K0)

    def half(g, read, write):
        kq, vq = Q_KV + 2 * g, Q_KV + 1 + 2 * g
        for s in range(SB):
            arrive(kq, s)
            arrive(vq, s)
        scores(g + 1, kq, write)
        attend(g, vq, read)

    def pair(gp, _):
        for e, (read, write) in enumerate(((sca, scb), (scb, sca))):
            g = 2 * gp + e
            half(g, read, write)
            last = (Q_VL - R - Q_KV) // 2

            @pl.when(g < last)
            def _():
                if R % 2 == 0:
                    issue_kv(k_hbm, g + 1 + R // 2, Q_KV + 2 * g + R)
                    issue_kv(v_hbm, g + R // 2, Q_KV + 1 + 2 * g + R)
                else:
                    issue_kv(v_hbm, g + R // 2, Q_KV + 2 * g + R)
                    issue_kv(k_hbm, g + 2 + R // 2, Q_KV + 1 + 2 * g + R)

            for n in range(last, GROUPS - 2):
                if n % 2 == e:
                    @pl.when(g == n)
                    def _(n=n):
                        issue(Q_KV + 2 * n + R)
                        issue(Q_KV + 1 + 2 * n + R)

        @pl.when(gp == EARLY // (2 * SB) - 1)
        def _():
            pl.semaphore_wait(barrier, 2)
            for i in range(NB):
                held_arrive(i)
            wo_steps(0)
            for c in range(NB // 2):
                stage2(0, c)
        return 0

    lax.fori_loop(0, GROUPS // 2 - 1, pair, 0)
    half(GROUPS - 2, sca, scb)
    issue(Q_KV + 2 * (GROUPS - 2) + R)
    issue(Q_KV + 1 + 2 * (GROUPS - 2) + R)
    for s in range(SB):
        arrive(Q_VL, s)
    attend(GROUPS - 1, Q_VL, scb)
    issue(Q_VL + R)

    wo_steps(1)
    for c in range(NB // 2):
        stage3(0, c)
    for c in range(NB // 2):
        stage2(1, c)
    for c in range(NB // 2):
        stage4(0, c)
        sent(0, c)
    for c in range(NB // 2):
        stage3(1, c)
    for c in range(NB // 2):
        stage4(1, c)
    normed(lambda j: y[0, j], 1)

    def gu_step(nb, _):
        gq, uq = Q_GU + 2 * nb, Q_GU + 1 + 2 * nb
        for s in range(SB):
            arrive(gq, s)
            arrive(uq, s)
        for n in range(2):
            cols = slice(n * TILE, (n + 1) * TILE)
            gate = up = None
            for kc in range(4):
                d = dot(lhs(kc), ring[slot(gq, kc), :, cols])
                gate = d if gate is None else gate + d
            for kc in range(4):
                d = dot(lhs(kc), ring[slot(uq, kc), :, cols])
                up = d if up is None else up + d
            hid[nb, :, cols] = (jax.nn.silu(gate) * up).astype(BF16)
        for n in range(NF):
            if Q_GU + 2 * n + R < Q_WD + NB:
                @pl.when(nb == n)
                def _(n=n):
                    issue(Q_GU + 2 * n + R)
                    issue(Q_GU + 1 + 2 * n + R)
        return 0

    lax.fori_loop(0, NF, gu_step, 0)

    def down(quad, cols):
        acc = None
        for kc in range(4):
            i = slot(quad, kc)
            if kc < 3:
                d = dot(jnp.concatenate([hid[2 * kc], hid[2 * kc + 1]], 1), ring[i, :, cols])
            else:
                d = dot(hid[NF - 1], ring[i, 0:FF - 3 * ROWS, cols])
            acc = d if acc is None else acc + d
        return acc

    def wd_step(c, _):
        for s in range(3):
            arrive(Q_WD + c, s)
        arrive(Q_WD + c, 3, FF - 3 * ROWS)
        for n in range(2):
            keep(1, 2 * c + n, slice(0, BATCH), down(Q_WD + c, slice(n * TILE, (n + 1) * TILE)))
        stage1(2, c)

        @pl.when(c >= 2)
        def _():
            stage2(2, c - 2)

        @pl.when(c >= 5)
        def _():
            stage3(2, c - 5)
        return 0

    for c in range(NB // 2):
        sent(1, c)
    lax.fori_loop(0, NB - 1, wd_step, 0)

    def finish(n):
        last_arrive(n)
        t = down(Q_WD + NB - 1, slice(n * TILE, (n + 1) * TILE))
        for h in range(2):
            fz[n, h] = t[:, h * 128:(h + 1) * 128]
            sz[n, h] = t[:, h * 128:(h + 1) * 128].astype(BF16)
        stage1(3, n)

    finish(0)
    stage2(2, NB - 3)
    finish(1)
    stage2(2, NB - 2)
    stage2(3, 0)
    stage3(2, NB - 6)
    stage3(2, NB - 5)
    stage2(3, 1)
    stage3(2, NB - 4)
    stage3(2, NB - 3)
    for c in range(NB - 4):
        stage4(2, c)
        sent(2, c)
    stage3(2, NB - 2)
    stage3(3, 0)
    stage4(2, NB - 4)
    stage4(2, NB - 3)
    stage3(3, 1)
    for c in range(NB - 4, NB - 1):
        if c == NB - 2:
            stage4(2, c)
        sent(2, c)
    for n in range(2):
        stage4(3, n)
    for n in range(2):
        sent(3, n)


def solution(mesh):
    half = HEAD // 2
    angle = (CACHE - 1) * float(THETA) ** (-np.arange(half) / half)
    turn = np.zeros((8, HEAD), np.float32)
    turn[0] = np.concatenate([np.cos(angle), np.cos(angle)])
    turn[1] = np.concatenate([-np.sin(angle), np.sin(angle)])
    hbm = pl.BlockSpec(memory_space=pl.ANY)

    def step(x, k_cache, v_cache, gain_a, wq, wo, gain_m, w_gate, w_up, w_down):
        flat = (BATCH, CACHE * KV, HEAD)
        dma = pltpu.SemaphoreType.DMA
        call = pl.pallas_call(
            kernel,
            out_shape=pltpu.VMEM((BATCH, D), BF16),
            in_specs=[hbm] * 11,
            out_specs=pl.BlockSpec(memory_space=pltpu.VMEM),
            scratch_shapes=[
                pltpu.VMEM((R * SB, ROWS, COLS), BF16),
                pltpu.VMEM((NB, ROWS, COLS), BF16),
                pltpu.VMEM((NT, BATCH, TILE), BF16),
                pltpu.VMEM((NT, BATCH, TILE), BF16),
                pltpu.VMEM((2, D // 128, 128), BF16),
                pltpu.VMEM((8, HEAD), F32),
                pltpu.VMEM((8 * BATCH, HEAD), F32),
                pltpu.VMEM((SB, 2, 16, ROWS), F32),
                pltpu.VMEM((SB, 2, 16, ROWS), F32),
                pltpu.VMEM((8 * BATCH, HEAD), F32),
                pltpu.VMEM((NF, BATCH, COLS), BF16),
                pltpu.VMEM((NT, BATCH, TILE), F32),
                pltpu.VMEM((2, NT, BATCH, TILE), BF16),
                pltpu.VMEM((2, NB, BATCH, TILE), BF16),
                pltpu.VMEM((2, NB, BATCH, TILE), BF16),
                pltpu.VMEM((2, NB, BATCH, TILE), BF16),
                pltpu.VMEM((2, NT, BATCH, TILE), BF16),
                pltpu.VMEM((2, 2, BATCH, 128), F32),
                pltpu.VMEM((2, 2, BATCH, 128), BF16),
                pltpu.VMEM((2, 3, BATCH, 128), BF16),
                pltpu.VMEM((2, 2, BATCH, 128), BF16),
                dma((R * SB,)), dma((NB,)), dma((2, SB)), dma((NT,)), dma((3,)),
                dma((3, 2 * NB + 2)), dma((3, 2 * NB + 2)),
            ],
            compiler_params=pltpu.CompilerParams(collective_id=0, has_side_effects=True, vmem_limit_bytes=65_900_000),
            cost_estimate=pl.CostEstimate(flops=20 * 10**9, bytes_accessed=240 * 10**6, transcendentals=0),
            name="layer",
        )
        return call(x, k_cache.reshape(flat), v_cache.reshape(flat), gain_a.reshape(D // 128, 128), wq, wo,
                    gain_m.reshape(D // 128, 128), w_gate, w_up, w_down, jnp.asarray(turn))

    states, cache, columns, rows_of = P("dp", None), P("dp", None, "tp", None), P(None, "tp"), P("tp", None)
    return jax.shard_map(
        step,
        mesh=mesh,
        in_specs=(states, cache, cache, P(None), columns, rows_of, P(None), columns, columns, rows_of),
        out_specs=states,
        check_vma=False,
    )
```

```python
import jax
import jax.numpy as jnp
import numpy as np
from jax import lax
from jax.experimental import pallas as pl
from jax.experimental.pallas import tpu as pltpu
from jax.sharding import PartitionSpec as P

HEAD = 128
THETA = 10000
BATCH = 64
CACHE = 2048
KV = 2
D = 4096
FF = 3584
ROWS, COLS = 1024, 512
SB = 4
R = 11
EARLY = 48
GROUPS = BATCH // SB
TILE = 256
NT = D // TILE
NB = D // COLS
NF = FF // COLS
Q_K0, Q_KV, Q_VL, Q_GU, Q_WD = 0, 1, 31, 32, 46
F32, BF16 = jnp.float32, jnp.bfloat16
NEG = float("-inf")


def kernel(x_hbm, k_hbm, v_hbm, ga_hbm, wq, wo, gm_hbm, wg, wu, wd, rot_hbm, out,
           ring, held, xb, ab, gb, rb, qb, sca, scb, seen, hid, f1, s1, r1, s2, r2, y,
           fz, sz, rz, yz, sem, dsem, wsem, lsem, xsem, gsem, xs, xr):
    tp = lax.axis_index("tp")
    k = lax.rem(tp, 2)
    sib = tp + 1 - 2 * k
    far = lax.rem(tp + 2, 4)

    def spot(quad):
        return quad % R if isinstance(quad, int) else lax.rem(quad, R)

    def slot(quad, s):
        return spot(quad) * SB + s

    def filled(ref, sem):
        pltpu.make_async_copy(ref, ref, sem).wait()

    def put(src, dst, s):
        pltpu.make_async_copy(src, dst, s).start(priority=1)

    def issue_wq():
        for i in range(2 * SB):
            pltpu.make_async_copy(wq.at[pl.ds(i % SB * ROWS, ROWS), pl.ds(i // SB * COLS, COLS)], held.at[i], wsem.at[i // SB]).start()

    def issue_kv(ref, g, quad):
        for s in range(SB):
            i = slot(quad, s)
            for c in range(4):
                put(ref.at[g * SB + s, pl.ds(c * ROWS, ROWS), :], ring.at[i, :, pl.ds(c * 128, 128)], sem.at[spot(quad)])

    def issue_wo():
        for i in range(NB):
            put(wo.at[:, pl.ds(i * COLS, COLS)], held.at[i], wsem.at[i // SB])

    def issue_gu(ref, nb, quad):
        for s in range(SB):
            i = slot(quad, s)
            cols = pl.ds(nb * COLS if isinstance(nb, int) else pl.multiple_of(nb * COLS, COLS), COLS)
            put(ref.at[pl.ds(s * ROWS, ROWS), cols], ring.at[i], sem.at[spot(quad)])

    def issue_last():
        for n in range(2):
            for s in range(SB):
                rows = ROWS if s < 3 else FF - 3 * ROWS
                put(wd.at[pl.ds(s * ROWS, rows), pl.ds((NT - 2 + n) * TILE, TILE)],
                    ring.at[slot(Q_WD + NB - 1, s), pl.ds(0, rows), pl.ds(n * TILE, TILE)], lsem.at[n, s // 3])

    def last_arrive(n):
        cols = pl.ds(n * TILE, TILE)
        filled(ring.at[pl.ds(slot(Q_WD + NB - 1, 0), 3), :, cols], lsem.at[n, 0])
        filled(ring.at[slot(Q_WD + NB - 1, 3), pl.ds(0, FF - 3 * ROWS), cols], lsem.at[n, 1])

    def issue_wd(nb):
        cols = pl.ds(nb * COLS if isinstance(nb, int) else pl.multiple_of(nb * COLS, COLS), COLS)
        for s in range(SB):
            i = slot(Q_WD + nb, s)
            if s < 3:
                put(wd.at[pl.ds(s * ROWS, ROWS), cols], ring.at[i], sem.at[spot(Q_WD + nb)])
            else:
                put(wd.at[pl.ds(s * ROWS, FF - 3 * ROWS), cols], ring.at[i, pl.ds(0, FF - 3 * ROWS), :], dsem.at[nb])

    def issue(quad):
        if quad == Q_K0:
            issue_kv(k_hbm, 0, quad)
        elif quad < Q_VL:
            g = (quad - Q_KV) // 2
            if (quad - Q_KV) % 2 == 0:
                issue_kv(k_hbm, g + 1, quad)
            else:
                issue_kv(v_hbm, g, quad)
        elif quad == Q_VL:
            issue_kv(v_hbm, GROUPS - 1, quad)
        elif quad < Q_WD:
            n = quad - Q_GU
            issue_gu(wg if n % 2 == 0 else wu, n // 2, quad)
        elif quad < Q_WD + NB - 1:
            issue_wd(quad - Q_WD)
        elif quad == Q_WD + NB - 1:
            issue_last()

    def arrive(quad, slots=SB):
        filled(ring.at[pl.ds(slot(quad, 0), slots)], sem.at[spot(quad)])

    def held_arrive(part):
        filled(held.at[pl.ds(part * SB, SB)], wsem.at[part])

    xcopies = [pltpu.make_async_copy(x_hbm.at[:, pl.ds(j * TILE, TILE)], xb.at[j], xsem) for j in range(NT)]
    small = [pltpu.make_async_copy(a, b, gsem.at[n]) for n, (a, b) in enumerate(
        ((ga_hbm, gb.at[0]), (gm_hbm, gb.at[1]), (rot_hbm, rb)))]
    for c in xcopies + small:
        c.start()
    issue_wq()
    for quad in range(R):
        issue(quad)

    barrier = pltpu.get_barrier_semaphore()
    for peer in (sib, far):
        pl.semaphore_signal(barrier, inc=1, device_id={"tp": peer}, device_id_type=pl.DeviceIdType.MESH)

    filled(xb, xsem)
    for c in small:
        c.wait()

    def normed(src, gain):
        total = jnp.zeros((BATCH, 128), F32)
        for j in range(NT):
            t = src(j).astype(F32)
            t = t * t
            total += t[:, :128] + t[:, 128:]
        scale = lax.rsqrt(jnp.sum(total, -1, keepdims=True) * (1.0 / D) + 1e-6)
        g = gb[gain].astype(F32)
        for j in range(NT):
            t = src(j).astype(F32)
            row = jnp.concatenate([g[2 * j:2 * j + 1], g[2 * j + 1:2 * j + 2]], 1)
            ab[j] = (t * scale * row).astype(BF16)

    def lhs(kc):
        return jnp.concatenate([ab[kc * 4 + t] for t in range(4)], 1)

    def dot(a, b):
        return jnp.dot(a, b, preferred_element_type=F32)

    normed(lambda j: xb[j], 0)

    cos, sin = rb[0:1, :], rb[1:2, :]
    for nc in range(2):
        held_arrive(nc)
        for n in range(2):
            acc = None
            for kc in range(4):
                d = dot(lhs(kc), held[nc * SB + kc, :, n * TILE:(n + 1) * TILE])
                acc = d if acc is None else acc + d
            for hh in range(2):
                t = acc[:, hh * HEAD:(hh + 1) * HEAD].astype(BF16).astype(F32)
                r = t * cos + pltpu.roll(t, HEAD // 2, 1) * sin
                head = nc * 4 + n * 2 + hh
                qb[head * BATCH:(head + 1) * BATCH, :] = r.astype(BF16).astype(F32)
    issue_wo()

    row = lax.broadcasted_iota(jnp.int32, (8, 128), 0)
    lane = lax.broadcasted_iota(jnp.int32, (8, 128), 1)
    mine = (lane % 2) == (row // 4)
    zero = jnp.zeros((8, HEAD), F32)
    rate = HEAD**-0.5 * float(np.log2(np.e))

    def scores(g, quad, sc):
        for s in range(SB):
            q = qb[pl.ds(g * SB + s, 8, stride=BATCH), :]
            qq = jnp.concatenate([jnp.concatenate([q, zero], 1), jnp.concatenate([zero, q], 1)], 0).astype(BF16)
            i = slot(quad, s)
            for h in range(2):
                sc[s, h] = lax.dot_general(qq, ring[i, :, h * TILE:(h + 1) * TILE], (((1,), (1,)), ((), ())),
                                           preferred_element_type=F32)

    def attend(g, quad, sc):
        for s in range(SB):
            i = slot(quad, s)
            p = {}
            top = None
            for h in range(2):
                for r in range(2):
                    for c in range(ROWS // 128):
                        t = jnp.where(mine, sc[s, h, r * 8:(r + 1) * 8, c * 128:(c + 1) * 128], NEG)
                        p[h, r, c] = t
                        top = t if top is None else jnp.maximum(top, t)
            top = jnp.max(top, -1, keepdims=True)
            total = None
            for key, t in p.items():
                e = jnp.exp2((t - top) * rate)
                p[key] = e
                total = e if total is None else total + e
            inv = 1.0 / jnp.sum(total, -1, keepdims=True)
            o = None
            for h in range(2):
                w = jnp.concatenate([jnp.concatenate([p[h, r, c] * inv for c in range(ROWS // 128)], 1)
                                     for r in range(2)], 0).astype(BF16)
                d = dot(w, ring[i, :, h * TILE:(h + 1) * TILE])
                o = d if o is None else o + d
            o = o[0:8, 0:HEAD] + o[8:16, HEAD:TILE]
            seen[pl.ds(g * SB + s, 8, stride=BATCH), :] = o.astype(BF16).astype(F32)

    def remote(src, dst, stage, n, peer):
        return pltpu.make_async_remote_copy(src_ref=src, dst_ref=dst, send_sem=xs.at[n], recv_sem=xr.at[stage, n],
                                            device_id={"tp": peer}, device_id_type=pl.DeviceIdType.MESH)

    class Unit:
        def __init__(self, e, c):
            self.e, self.c = e, c
            if e < 3:
                t = 4 if e < 2 else 1
                at = (pl.ds(0, EARLY), pl.ds(EARLY, BATCH - EARLY), pl.ds(0, BATCH))[e]
                p = e // 2
                own, other, got = pl.ds(2 * t * c + t * k, t), pl.ds(2 * t * c + t * (1 - k), t), pl.ds(t * c, t)
                self.n = (0, 2, 4)[e] + c
                self.term, self.give, self.take = f1.at[own, at], s1.at[p, other, at], r1.at[p, got, at]
                self.pair, self.far = s2.at[p, got, at], r2.at[p, got, at]
                self.base = xb.at[own, at] if e < 2 else y.at[0, own]
                self.result = y.at[p, own, at]
            else:
                self.n = NB + 3 + c
                half = pl.ds(pl.multiple_of(k * 128, 128), 128)
                self.term, self.give, self.take = fz.at[c, k], sz.at[c, 1 - k], rz.at[c, 0]
                self.pair, self.far = rz.at[c, 1], rz.at[c, 2]
                self.base, self.result = y.at[0, NT - 2 + c, :, half], yz.at[c, k]

        def copy1(self):
            return remote(self.give, self.take, 0, self.n, sib)

        def copy2(self):
            return remote(self.pair, self.far, 1, self.n, far)

        def copy3(self):
            return remote(self.result, self.result, 2, self.n, sib)

    def stage1(e, c):
        Unit(e, c).copy1().start()

    def stage2(e, c):
        u = Unit(e, c)
        u.copy1().wait_recv()
        u.pair[...] = (u.term[...] + u.take[...].astype(F32)).astype(BF16)
        u.copy1().wait_send()
        u.copy2().start()

    def stage3(e, c):
        u = Unit(e, c)
        u.copy2().wait_recv()
        u.result[...] = (u.base[...].astype(F32) + (u.pair[...].astype(F32) + u.far[...].astype(F32))).astype(BF16)
        u.copy2().wait_send()
        u.copy3().start()

    def stage4(e, c):
        Unit(e, c).copy3().wait_recv()
        if e == 2:
            for j in (2 * c, 2 * c + 1):
                out[:, j * TILE:(j + 1) * TILE] = y[1, j]
        elif e == 3:
            for n in range(2):
                out[:, (NT - 2 + c) * TILE + n * 128:(NT - 2 + c) * TILE + (n + 1) * 128] = yz[c, n]

    def sent(e, c):
        Unit(e, c).copy3().wait_send()

    def keep(p, j, at, t):
        f1[j, at] = t
        s1[p, j, at] = t.astype(BF16)

    def wo_steps(e):
        at = slice(0, EARLY) if e == 0 else slice(EARLY, BATCH)
        a = jnp.concatenate([seen[h * BATCH + at.start:h * BATCH + at.stop, :].astype(BF16) for h in range(8)], 1)
        for j in range(NT):
            keep(0, j, at, dot(a, held[j // 2, :, j % 2 * TILE:(j % 2 + 1) * TILE]))
            if j % 8 == 7:
                stage1(e, j // 8)

    arrive(Q_K0)
    scores(0, Q_K0, sca)
    issue(R + Q_K0)

    def half(g, read, write):
        kq, vq = Q_KV + 2 * g, Q_KV + 1 + 2 * g
        arrive(kq)
        arrive(vq)
        scores(g + 1, kq, write)
        attend(g, vq, read)

    def pair(gp, _):
        for e, (read, write) in enumerate(((sca, scb), (scb, sca))):
            g = 2 * gp + e
            half(g, read, write)
            last = (Q_VL - R - Q_KV) // 2

            @pl.when(g < last)
            def _():
                if R % 2 == 0:
                    issue_kv(k_hbm, g + 1 + R // 2, Q_KV + 2 * g + R)
                    issue_kv(v_hbm, g + R // 2, Q_KV + 1 + 2 * g + R)
                else:
                    issue_kv(v_hbm, g + R // 2, Q_KV + 2 * g + R)
                    issue_kv(k_hbm, g + 2 + R // 2, Q_KV + 1 + 2 * g + R)

            for n in range(last, GROUPS - 2):
                if n % 2 == e:
                    @pl.when(g == n)
                    def _(n=n):
                        issue(Q_KV + 2 * n + R)
                        issue(Q_KV + 1 + 2 * n + R)

        @pl.when(gp == EARLY // (2 * SB) - 1)
        def _():
            pl.semaphore_wait(barrier, 2)
            held_arrive(0)
            held_arrive(1)
            wo_steps(0)
            for c in range(2):
                stage2(0, c)
        return 0

    lax.fori_loop(0, GROUPS // 2 - 1, pair, 0)
    half(GROUPS - 2, sca, scb)
    issue(Q_KV + 2 * (GROUPS - 2) + R)
    issue(Q_KV + 1 + 2 * (GROUPS - 2) + R)
    arrive(Q_VL)
    attend(GROUPS - 1, Q_VL, scb)
    issue(Q_VL + R)

    wo_steps(1)
    for c in range(2):
        stage3(0, c)
    for c in range(2):
        stage2(1, c)
    for c in range(2):
        stage4(0, c)
        sent(0, c)
    for c in range(2):
        stage3(1, c)
    for c in range(2):
        stage4(1, c)
    normed(lambda j: y[0, j], 1)

    def gu_step(nb, _):
        gq, uq = Q_GU + 2 * nb, Q_GU + 1 + 2 * nb
        arrive(gq)
        arrive(uq)
        for n in range(2):
            cols = slice(n * TILE, (n + 1) * TILE)
            gate = up = None
            for kc in range(4):
                d = dot(lhs(kc), ring[slot(gq, kc), :, cols])
                gate = d if gate is None else gate + d
            for kc in range(4):
                d = dot(lhs(kc), ring[slot(uq, kc), :, cols])
                up = d if up is None else up + d
            hid[nb, :, cols] = (jax.nn.silu(gate) * up).astype(BF16)
        for n in range(NF):
            if Q_GU + 2 * n + R < Q_WD + NB:
                @pl.when(nb == n)
                def _(n=n):
                    issue(Q_GU + 2 * n + R)
                    issue(Q_GU + 1 + 2 * n + R)
        return 0

    lax.fori_loop(0, NF, gu_step, 0)

    def down(quad, cols):
        parts = []
        for kc in range(4):
            i = slot(quad, kc)
            if kc < 3:
                parts.append(dot(jnp.concatenate([hid[2 * kc], hid[2 * kc + 1]], 1), ring[i, :, cols]))
            else:
                parts.append(dot(hid[NF - 1], ring[i, 0:FF - 3 * ROWS, cols]))
        return parts[0] + parts[1], parts[2] + parts[3]

    def wd_step(c, _):
        arrive(Q_WD + c, 3)
        filled(ring.at[slot(Q_WD + c, 3), pl.ds(0, FF - 3 * ROWS)], dsem.at[c])
        for n in range(2):
            keep(1, 2 * c + n, slice(0, BATCH), sum(down(Q_WD + c, slice(n * TILE, (n + 1) * TILE))))
        stage1(2, c)

        @pl.when(c >= 1)
        def _():
            stage2(2, c - 1)
        return 0

    for c in range(2):
        sent(1, c)
    lax.fori_loop(0, NB - 1, wd_step, 0)

    def finish(n):
        a, b = down(Q_WD + NB - 1, slice(n * TILE, (n + 1) * TILE))
        t = a + jnp.where(k >= 0, b, 0.0)
        for h in range(2):
            fz[n, h] = t[:, h * 128:(h + 1) * 128]
            sz[n, h] = t[:, h * 128:(h + 1) * 128].astype(BF16)
        stage1(3, n)

    last_arrive(0)
    finish(0)
    last_arrive(1)
    finish(1)
    stage2(2, NB - 2)
    stage2(3, 0)
    for c in range(NB - 4):
        stage3(2, c)
    stage2(3, 1)
    stage3(2, NB - 4)
    stage3(2, NB - 3)
    for c in range(NB - 4):
        stage4(2, c)
    stage3(2, NB - 2)
    stage3(3, 0)
    stage4(2, NB - 4)
    stage4(2, NB - 3)
    stage3(3, 1)
    stage4(2, NB - 2)
    for n in range(2):
        stage4(3, n)
    for c in range(NB - 1):
        sent(2, c)
    for n in range(2):
        sent(3, n)


def solution(mesh):
    half = HEAD // 2
    angle = (CACHE - 1) * float(THETA) ** (-np.arange(half) / half)
    turn = np.zeros((8, HEAD), np.float32)
    turn[0] = np.concatenate([np.cos(angle), np.cos(angle)])
    turn[1] = np.concatenate([-np.sin(angle), np.sin(angle)])
    hbm = pl.BlockSpec(memory_space=pl.ANY)

    def step(x, k_cache, v_cache, gain_a, wq, wo, gain_m, w_gate, w_up, w_down):
        flat = (BATCH, CACHE * KV, HEAD)
        dma = pltpu.SemaphoreType.DMA
        call = pl.pallas_call(
            kernel,
            out_shape=pltpu.VMEM((BATCH, D), BF16),
            in_specs=[hbm] * 11,
            out_specs=pl.BlockSpec(memory_space=pltpu.VMEM),
            scratch_shapes=[
                pltpu.VMEM((R * SB, ROWS, COLS), BF16),
                pltpu.VMEM((NB, ROWS, COLS), BF16),
                pltpu.VMEM((NT, BATCH, TILE), BF16),
                pltpu.VMEM((NT, BATCH, TILE), BF16),
                pltpu.VMEM((2, D // 128, 128), BF16),
                pltpu.VMEM((8, HEAD), F32),
                pltpu.VMEM((8 * BATCH, HEAD), F32),
                pltpu.VMEM((SB, 2, 16, ROWS), F32),
                pltpu.VMEM((SB, 2, 16, ROWS), F32),
                pltpu.VMEM((8 * BATCH, HEAD), F32),
                pltpu.VMEM((NF, BATCH, COLS), BF16),
                pltpu.VMEM((NT, BATCH, TILE), F32),
                pltpu.VMEM((2, NT, BATCH, TILE), BF16),
                pltpu.VMEM((2, NB, BATCH, TILE), BF16),
                pltpu.VMEM((2, NB, BATCH, TILE), BF16),
                pltpu.VMEM((2, NB, BATCH, TILE), BF16),
                pltpu.VMEM((2, NT, BATCH, TILE), BF16),
                pltpu.VMEM((2, 2, BATCH, 128), F32),
                pltpu.VMEM((2, 2, BATCH, 128), BF16),
                pltpu.VMEM((2, 3, BATCH, 128), BF16),
                pltpu.VMEM((2, 2, BATCH, 128), BF16),
                dma((R,)), dma((NB - 1,)), dma((2,)), dma((2, 2)), dma(()), dma((3,)),
                dma((NB + 5,)), dma((3, NB + 5)),
            ],
            compiler_params=pltpu.CompilerParams(collective_id=0, has_side_effects=True, vmem_limit_bytes=65_900_000),
            cost_estimate=pl.CostEstimate(flops=20 * 10**9, bytes_accessed=240 * 10**6, transcendentals=0),
            name="layer",
        )
        return call(x, k_cache.reshape(flat), v_cache.reshape(flat), gain_a.reshape(D // 128, 128), wq, wo,
                    gain_m.reshape(D // 128, 128), w_gate, w_up, w_down, jnp.asarray(turn))

    states, cache, columns, rows_of = P("dp", None), P("dp", None, "tp", None), P(None, "tp"), P("tp", None)
    return jax.shard_map(
        step,
        mesh=mesh,
        in_specs=(states, cache, cache, P(None), columns, rows_of, P(None), columns, columns, rows_of),
        out_specs=states,
        check_vma=False,
    )
```

```python
import jax
import jax.numpy as jnp
import numpy as np
from jax import lax
from jax.experimental import pallas as pl
from jax.experimental.pallas import tpu as pltpu
from jax.sharding import PartitionSpec as P

HEAD = 128
THETA = 10000
BATCH = 64
CACHE = 2048
KV = 2
D = 4096
FF = 3584
ROWS, COLS = 1024, 512
SB = 4
R = 11
EARLY = 48
GROUPS = BATCH // SB
TILE = 256
NT = D // TILE
NB = D // COLS
NF = FF // COLS
Q_K0, Q_KV, Q_VL, Q_GU, Q_WD = 0, 1, 31, 32, 46
F32, BF16 = jnp.float32, jnp.bfloat16
NEG = float("-inf")


def kernel(x_hbm, k_hbm, v_hbm, ga_hbm, wq, wo, gm_hbm, wg, wu, wd, rot_hbm, out,
           ring, held, xb, ab, gb, rb, qb, sca, scb, seen, hid, f1, s1, r1, s2, r2, y,
           fz, sz, rz, yz, sem, dsem, wsem, lsem, xsem, gsem, xs, xr):
    tp = lax.axis_index("tp")
    k = lax.rem(tp, 2)
    sib = tp + 1 - 2 * k
    far = lax.rem(tp + 2, 4)

    def spot(quad):
        return quad % R if isinstance(quad, int) else lax.rem(quad, R)

    def slot(quad, s):
        return spot(quad) * SB + s

    def filled(ref, sem):
        pltpu.make_async_copy(ref, ref, sem).wait()

    def put(src, dst, s):
        pltpu.make_async_copy(src, dst, s).start(priority=1)

    def issue_wq():
        for i in range(2 * SB):
            pltpu.make_async_copy(wq.at[pl.ds(i % SB * ROWS, ROWS), pl.ds(i // SB * COLS, COLS)], held.at[i], wsem.at[i // SB]).start()

    def issue_kv(ref, g, quad):
        for s in range(SB):
            i = slot(quad, s)
            for c in range(4):
                put(ref.at[g * SB + s, pl.ds(c * ROWS, ROWS), :], ring.at[i, :, pl.ds(c * 128, 128)], sem.at[spot(quad)])

    def issue_wo():
        for i in range(NB):
            put(wo.at[:, pl.ds(i * COLS, COLS)], held.at[i], wsem.at[i // SB])

    def issue_gu(ref, nb, quad):
        for s in range(SB):
            i = slot(quad, s)
            cols = pl.ds(nb * COLS if isinstance(nb, int) else pl.multiple_of(nb * COLS, COLS), COLS)
            put(ref.at[pl.ds(s * ROWS, ROWS), cols], ring.at[i], sem.at[spot(quad)])

    def issue_last():
        for n in range(2):
            for s in range(SB):
                rows = ROWS if s < 3 else FF - 3 * ROWS
                put(wd.at[pl.ds(s * ROWS, rows), pl.ds((NT - 2 + n) * TILE, TILE)],
                    ring.at[slot(Q_WD + NB - 1, s), pl.ds(0, rows), pl.ds(n * TILE, TILE)], lsem.at[n, s // 3])

    def last_arrive(n):
        cols = pl.ds(n * TILE, TILE)
        filled(ring.at[pl.ds(slot(Q_WD + NB - 1, 0), 3), :, cols], lsem.at[n, 0])
        filled(ring.at[slot(Q_WD + NB - 1, 3), pl.ds(0, FF - 3 * ROWS), cols], lsem.at[n, 1])

    def issue_wd(nb):
        cols = pl.ds(nb * COLS if isinstance(nb, int) else pl.multiple_of(nb * COLS, COLS), COLS)
        for s in range(SB):
            i = slot(Q_WD + nb, s)
            if s < 3:
                put(wd.at[pl.ds(s * ROWS, ROWS), cols], ring.at[i], sem.at[spot(Q_WD + nb)])
            else:
                put(wd.at[pl.ds(s * ROWS, FF - 3 * ROWS), cols], ring.at[i, pl.ds(0, FF - 3 * ROWS), :], dsem.at[nb])

    def issue(quad):
        if quad == Q_K0:
            issue_kv(k_hbm, 0, quad)
        elif quad < Q_VL:
            g = (quad - Q_KV) // 2
            if (quad - Q_KV) % 2 == 0:
                issue_kv(k_hbm, g + 1, quad)
            else:
                issue_kv(v_hbm, g, quad)
        elif quad == Q_VL:
            issue_kv(v_hbm, GROUPS - 1, quad)
        elif quad < Q_WD:
            n = quad - Q_GU
            issue_gu(wg if n % 2 == 0 else wu, n // 2, quad)
        elif quad < Q_WD + NB - 1:
            issue_wd(quad - Q_WD)
        elif quad == Q_WD + NB - 1:
            issue_last()

    def arrive(quad, slots=SB):
        filled(ring.at[pl.ds(slot(quad, 0), slots)], sem.at[spot(quad)])

    def held_arrive(part):
        filled(held.at[pl.ds(part * SB, SB)], wsem.at[part])

    xcopies = [pltpu.make_async_copy(x_hbm.at[:, pl.ds(j * TILE, TILE)], xb.at[j], xsem) for j in range(NT)]
    small = [pltpu.make_async_copy(a, b, gsem.at[n]) for n, (a, b) in enumerate(
        ((ga_hbm, gb.at[0]), (gm_hbm, gb.at[1]), (rot_hbm, rb)))]
    for c in xcopies + small:
        c.start()
    issue_wq()
    for quad in range(R):
        issue(quad)

    barrier = pltpu.get_barrier_semaphore()
    for peer in (sib, far):
        pl.semaphore_signal(barrier, inc=1, device_id={"tp": peer}, device_id_type=pl.DeviceIdType.MESH)

    filled(xb, xsem)
    for c in small:
        c.wait()

    def normed(src, gain):
        total = jnp.zeros((BATCH, 128), F32)
        for j in range(NT):
            t = src(j).astype(F32)
            t = t * t
            total += t[:, :128] + t[:, 128:]
        scale = lax.rsqrt(jnp.sum(total, -1, keepdims=True) * (1.0 / D) + 1e-6)
        g = gb[gain].astype(F32)
        for j in range(NT):
            t = src(j).astype(F32)
            row = jnp.concatenate([g[2 * j:2 * j + 1], g[2 * j + 1:2 * j + 2]], 1)
            ab[j] = (t * scale * row).astype(BF16)

    def lhs(kc):
        return jnp.concatenate([ab[kc * 4 + t] for t in range(4)], 1)

    def dot(a, b):
        return jnp.dot(a, b, preferred_element_type=F32)

    normed(lambda j: xb[j], 0)

    cos, sin = rb[0:1, :], rb[1:2, :]
    for nc in range(2):
        held_arrive(nc)
        for n in range(2):
            acc = None
            for kc in range(4):
                d = dot(lhs(kc), held[nc * SB + kc, :, n * TILE:(n + 1) * TILE])
                acc = d if acc is None else acc + d
            for hh in range(2):
                t = acc[:, hh * HEAD:(hh + 1) * HEAD].astype(BF16).astype(F32)
                r = t * cos + pltpu.roll(t, HEAD // 2, 1) * sin
                head = nc * 4 + n * 2 + hh
                qb[head * BATCH:(head + 1) * BATCH, :] = r.astype(BF16).astype(F32)
    issue_wo()

    row = lax.broadcasted_iota(jnp.int32, (8, 128), 0)
    lane = lax.broadcasted_iota(jnp.int32, (8, 128), 1)
    mine = (lane % 2) == (row // 4)
    zero = jnp.zeros((8, HEAD), F32)
    rate = HEAD**-0.5 * float(np.log2(np.e))

    def scores(g, quad, sc):
        for s in range(SB):
            q = qb[pl.ds(g * SB + s, 8, stride=BATCH), :]
            qq = jnp.concatenate([jnp.concatenate([q, zero], 1), jnp.concatenate([zero, q], 1)], 0).astype(BF16)
            i = slot(quad, s)
            for h in range(2):
                sc[s, h] = lax.dot_general(qq, ring[i, :, h * TILE:(h + 1) * TILE], (((1,), (1,)), ((), ())),
                                           preferred_element_type=F32)

    def attend(g, quad, sc):
        for s in range(SB):
            i = slot(quad, s)
            p = {}
            top = None
            for h in range(2):
                for r in range(2):
                    for c in range(ROWS // 128):
                        t = jnp.where(mine, sc[s, h, r * 8:(r + 1) * 8, c * 128:(c + 1) * 128], NEG)
                        p[h, r, c] = t
                        top = t if top is None else jnp.maximum(top, t)
            top = jnp.max(top, -1, keepdims=True)
            total = None
            for key, t in p.items():
                e = jnp.exp2((t - top) * rate)
                p[key] = e
                total = e if total is None else total + e
            inv = 1.0 / jnp.sum(total, -1, keepdims=True)
            o = None
            for h in range(2):
                w = jnp.concatenate([jnp.concatenate([p[h, r, c] * inv for c in range(ROWS // 128)], 1)
                                     for r in range(2)], 0).astype(BF16)
                d = dot(w, ring[i, :, h * TILE:(h + 1) * TILE])
                o = d if o is None else o + d
            o = o[0:8, 0:HEAD] + o[8:16, HEAD:TILE]
            seen[pl.ds(g * SB + s, 8, stride=BATCH), :] = o.astype(BF16).astype(F32)

    def remote(src, dst, stage, n, peer):
        return pltpu.make_async_remote_copy(src_ref=src, dst_ref=dst, send_sem=xs.at[n], recv_sem=xr.at[stage, n],
                                            device_id={"tp": peer}, device_id_type=pl.DeviceIdType.MESH)

    class Unit:
        def __init__(self, e, c):
            self.e, self.c = e, c
            if e < 3:
                t = 4 if e < 2 else 1
                at = (pl.ds(0, EARLY), pl.ds(EARLY, BATCH - EARLY), pl.ds(0, BATCH))[e]
                p = e // 2
                own, other, got = pl.ds(2 * t * c + t * k, t), pl.ds(2 * t * c + t * (1 - k), t), pl.ds(t * c, t)
                self.n = (0, 2, 4)[e] + c
                self.term, self.give, self.take = f1.at[own, at], s1.at[p, other, at], r1.at[p, got, at]
                self.pair, self.far = s2.at[p, got, at], r2.at[p, got, at]
                self.base = xb.at[own, at] if e < 2 else y.at[0, own]
                self.result = y.at[p, own, at]
            else:
                self.n = NB + 3 + c
                half = pl.ds(pl.multiple_of(k * 128, 128), 128)
                self.term, self.give, self.take = fz.at[c, k], sz.at[c, 1 - k], rz.at[c, 0]
                self.pair, self.far = rz.at[c, 1], rz.at[c, 2]
                self.base, self.result = y.at[0, NT - 2 + c, :, half], yz.at[c, k]

        def copy1(self):
            return remote(self.give, self.take, 0, self.n, sib)

        def copy2(self):
            return remote(self.pair, self.far, 1, self.n, far)

        def copy3(self):
            return remote(self.result, self.result, 2, self.n, sib)

    def stage1(e, c):
        Unit(e, c).copy1().start()

    def stage2(e, c):
        u = Unit(e, c)
        u.copy1().wait_recv()
        u.pair[...] = (u.term[...] + u.take[...].astype(F32)).astype(BF16)
        u.copy1().wait_send()
        u.copy2().start()

    def stage3(e, c):
        u = Unit(e, c)
        u.copy2().wait_recv()
        u.result[...] = (u.base[...].astype(F32) + (u.pair[...].astype(F32) + u.far[...].astype(F32))).astype(BF16)
        u.copy2().wait_send()
        u.copy3().start()

    def stage4(e, c):
        Unit(e, c).copy3().wait_recv()
        if e == 2:
            for j in (2 * c, 2 * c + 1):
                out[:, j * TILE:(j + 1) * TILE] = y[1, j]
        elif e == 3:
            for n in range(2):
                out[:, (NT - 2 + c) * TILE + n * 128:(NT - 2 + c) * TILE + (n + 1) * 128] = yz[c, n]

    def sent(e, c):
        Unit(e, c).copy3().wait_send()

    def keep(p, j, at, t):
        f1[j, at] = t
        s1[p, j, at] = t.astype(BF16)

    def wo_steps(e):
        at = slice(0, EARLY) if e == 0 else slice(EARLY, BATCH)
        a = jnp.concatenate([seen[h * BATCH + at.start:h * BATCH + at.stop, :].astype(BF16) for h in range(8)], 1)
        for j in range(NT):
            keep(0, j, at, dot(a, held[j // 2, :, j % 2 * TILE:(j % 2 + 1) * TILE]))
            if j % 8 == 7:
                stage1(e, j // 8)

    arrive(Q_K0)
    scores(0, Q_K0, sca)
    issue(R + Q_K0)

    def half(g, read, write):
        kq, vq = Q_KV + 2 * g, Q_KV + 1 + 2 * g
        arrive(kq)
        arrive(vq)
        scores(g + 1, kq, write)
        attend(g, vq, read)

    def pair(gp, _):
        for e, (read, write) in enumerate(((sca, scb), (scb, sca))):
            g = 2 * gp + e
            half(g, read, write)
            last = (Q_VL - R - Q_KV) // 2

            @pl.when(g < last)
            def _():
                if R % 2 == 0:
                    issue_kv(k_hbm, g + 1 + R // 2, Q_KV + 2 * g + R)
                    issue_kv(v_hbm, g + R // 2, Q_KV + 1 + 2 * g + R)
                else:
                    issue_kv(v_hbm, g + R // 2, Q_KV + 2 * g + R)
                    issue_kv(k_hbm, g + 2 + R // 2, Q_KV + 1 + 2 * g + R)

            for n in range(last, GROUPS - 2):
                if n % 2 == e:
                    @pl.when(g == n)
                    def _(n=n):
                        issue(Q_KV + 2 * n + R)
                        issue(Q_KV + 1 + 2 * n + R)

        @pl.when(gp == EARLY // (2 * SB) - 1)
        def _():
            pl.semaphore_wait(barrier, 2)
            held_arrive(0)
            held_arrive(1)
            wo_steps(0)
            for c in range(2):
                stage2(0, c)
        return 0

    lax.fori_loop(0, GROUPS // 2 - 1, pair, 0)
    half(GROUPS - 2, sca, scb)
    issue(Q_KV + 2 * (GROUPS - 2) + R)
    issue(Q_KV + 1 + 2 * (GROUPS - 2) + R)
    arrive(Q_VL)
    attend(GROUPS - 1, Q_VL, scb)
    issue(Q_VL + R)

    wo_steps(1)
    for c in range(2):
        stage3(0, c)
    for c in range(2):
        stage2(1, c)
    for c in range(2):
        stage4(0, c)
        sent(0, c)
    for c in range(2):
        stage3(1, c)
    for c in range(2):
        stage4(1, c)
    normed(lambda j: y[0, j], 1)

    def gu_step(nb, _):
        gq, uq = Q_GU + 2 * nb, Q_GU + 1 + 2 * nb
        arrive(gq)
        arrive(uq)
        for n in range(2):
            cols = slice(n * TILE, (n + 1) * TILE)
            gate = up = None
            for kc in range(4):
                d = dot(lhs(kc), ring[slot(gq, kc), :, cols])
                gate = d if gate is None else gate + d
            for kc in range(4):
                d = dot(lhs(kc), ring[slot(uq, kc), :, cols])
                up = d if up is None else up + d
            hid[nb, :, cols] = (jax.nn.silu(gate) * up).astype(BF16)
        for n in range(NF):
            if Q_GU + 2 * n + R < Q_WD + NB:
                @pl.when(nb == n)
                def _(n=n):
                    issue(Q_GU + 2 * n + R)
                    issue(Q_GU + 1 + 2 * n + R)
        return 0

    lax.fori_loop(0, NF, gu_step, 0)

    def down(quad, cols):
        parts = []
        for kc in range(4):
            i = slot(quad, kc)
            if kc < 3:
                parts.append(dot(jnp.concatenate([hid[2 * kc], hid[2 * kc + 1]], 1), ring[i, :, cols]))
            else:
                parts.append(dot(hid[NF - 1], ring[i, 0:FF - 3 * ROWS, cols]))
        return parts[0] + parts[1], parts[2] + parts[3]

    def wd_step(c, _):
        arrive(Q_WD + c, 3)
        filled(ring.at[slot(Q_WD + c, 3), pl.ds(0, FF - 3 * ROWS)], dsem.at[c])
        for n in range(2):
            keep(1, 2 * c + n, slice(0, BATCH), sum(down(Q_WD + c, slice(n * TILE, (n + 1) * TILE))))
        stage1(2, c)

        @pl.when(c >= 1)
        def _():
            stage2(2, c - 1)
        return 0

    for c in range(2):
        sent(1, c)
    lax.fori_loop(0, NB - 1, wd_step, 0)

    def finish(n):
        a, b = down(Q_WD + NB - 1, slice(n * TILE, (n + 1) * TILE))
        t = a + jnp.where(k >= 0, b, 0.0)
        for h in range(2):
            fz[n, h] = t[:, h * 128:(h + 1) * 128]
            sz[n, h] = t[:, h * 128:(h + 1) * 128].astype(BF16)
        stage1(3, n)

    last_arrive(0)
    finish(0)
    last_arrive(1)
    finish(1)
    for c in range(NB - 4):
        stage3(2, c)
    stage2(2, NB - 2)
    stage2(3, 0)
    stage2(3, 1)
    stage3(2, NB - 4)
    stage3(2, NB - 3)
    for c in range(NB - 4):
        stage4(2, c)
    stage3(2, NB - 2)
    stage3(3, 0)
    stage4(2, NB - 4)
    stage4(2, NB - 3)
    stage3(3, 1)
    stage4(2, NB - 2)
    for n in range(2):
        stage4(3, n)
    for c in range(NB - 1):
        sent(2, c)
    for n in range(2):
        sent(3, n)


def solution(mesh):
    half = HEAD // 2
    angle = (CACHE - 1) * float(THETA) ** (-np.arange(half) / half)
    turn = np.zeros((8, HEAD), np.float32)
    turn[0] = np.concatenate([np.cos(angle), np.cos(angle)])
    turn[1] = np.concatenate([-np.sin(angle), np.sin(angle)])
    hbm = pl.BlockSpec(memory_space=pl.ANY)

    def step(x, k_cache, v_cache, gain_a, wq, wo, gain_m, w_gate, w_up, w_down):
        flat = (BATCH, CACHE * KV, HEAD)
        dma = pltpu.SemaphoreType.DMA
        call = pl.pallas_call(
            kernel,
            out_shape=pltpu.VMEM((BATCH, D), BF16),
            in_specs=[hbm] * 11,
            out_specs=pl.BlockSpec(memory_space=pltpu.VMEM),
            scratch_shapes=[
                pltpu.VMEM((R * SB, ROWS, COLS), BF16),
                pltpu.VMEM((NB, ROWS, COLS), BF16),
                pltpu.VMEM((NT, BATCH, TILE), BF16),
                pltpu.VMEM((NT, BATCH, TILE), BF16),
                pltpu.VMEM((2, D // 128, 128), BF16),
                pltpu.VMEM((8, HEAD), F32),
                pltpu.VMEM((8 * BATCH, HEAD), F32),
                pltpu.VMEM((SB, 2, 16, ROWS), F32),
                pltpu.VMEM((SB, 2, 16, ROWS), F32),
                pltpu.VMEM((8 * BATCH, HEAD), F32),
                pltpu.VMEM((NF, BATCH, COLS), BF16),
                pltpu.VMEM((NT, BATCH, TILE), F32),
                pltpu.VMEM((2, NT, BATCH, TILE), BF16),
                pltpu.VMEM((2, NB, BATCH, TILE), BF16),
                pltpu.VMEM((2, NB, BATCH, TILE), BF16),
                pltpu.VMEM((2, NB, BATCH, TILE), BF16),
                pltpu.VMEM((2, NT, BATCH, TILE), BF16),
                pltpu.VMEM((2, 2, BATCH, 128), F32),
                pltpu.VMEM((2, 2, BATCH, 128), BF16),
                pltpu.VMEM((2, 3, BATCH, 128), BF16),
                pltpu.VMEM((2, 2, BATCH, 128), BF16),
                dma((R,)), dma((NB - 1,)), dma((2,)), dma((2, 2)), dma(()), dma((3,)),
                dma((NB + 5,)), dma((3, NB + 5)),
            ],
            compiler_params=pltpu.CompilerParams(collective_id=0, has_side_effects=True, vmem_limit_bytes=65_900_000),
            cost_estimate=pl.CostEstimate(flops=20 * 10**9, bytes_accessed=240 * 10**6, transcendentals=0),
            name="layer",
        )
        return call(x, k_cache.reshape(flat), v_cache.reshape(flat), gain_a.reshape(D // 128, 128), wq, wo,
                    gain_m.reshape(D // 128, 128), w_gate, w_up, w_down, jnp.asarray(turn))

    states, cache, columns, rows_of = P("dp", None), P("dp", None, "tp", None), P(None, "tp"), P("tp", None)
    return jax.shard_map(
        step,
        mesh=mesh,
        in_specs=(states, cache, cache, P(None), columns, rows_of, P(None), columns, columns, rows_of),
        out_specs=states,
        check_vma=False,
    )
```
